32 devices in a mesh: dp: 1 (over z), ey: 4 (over y), ex: 4 (over x), core: 2 (over core).
Axes of the slice: x: 4, y: 4, z: 1, core: 2. Of those that a mesh axis runs over, the one named last changes fastest.
The devices are a block of a 4x4x8 slice.
Arguments:
- tokens: bfloat16 [24576, 2048], P(('dp', 'ey', 'ex', 'core'))
- expert_ids: int32 [24576, 8], P(('dp', 'ey', 'ex', 'core'))
- gate_prob: float32 [24576, 8], P(('dp', 'ey', 'ex', 'core'))
- w_gate: bfloat16 [64, 2048, 1024], P(('ey', 'ex', 'core'))
- w_up: bfloat16 [64, 2048, 1024], P(('ey', 'ex', 'core'))
- w_down: bfloat16 [64, 1024, 2048], P(('ey', 'ex', 'core'))
Outputs:
- output: bfloat16 [24576, 2048], P(('dp', 'ey', 'ex', 'core'))
All inputs are finite; a program needn't handle non-finite values.
Results may differ from the reference program's by a relative error of at most 0.0116772.
Values are sent between devices in bfloat16 or wider.
A program may use at most 768 MiB of HBM per device.

```python
import jax
import jax.numpy as jnp
import numpy as np
from jax import lax

D_MODEL = 2048
D_FF = 1024
EXPERTS = 64
TOP_K = 8
BASE_ROWS = 64
GRID_Y = 4
GRID_X = 4
CORES = 2

GROUP_DEVS = GRID_Y * GRID_X * CORES
TOK_DEV = 3 * EXPERTS * BASE_ROWS // (2 * TOP_K)
EXP_DEV = EXPERTS // GROUP_DEVS
HOT_ROWS = GRID_Y * GRID_X * BASE_ROWS // 2


def sorted_lists():
    dev_ids = np.arange(GROUP_DEVS)
    chip_y = dev_ids // CORES // GRID_X
    chip_x = (dev_ids // CORES) % GRID_X
    half_y = GRID_Y // 2
    half_x = GRID_X // 2
    first_hot = (chip_y == 0) & (chip_x < half_x)
    second_hot = (chip_y == half_y) & (chip_x >= half_x)
    dst_chip = np.where(first_hot, half_y * GRID_X + chip_x + half_x, np.where(second_hot, chip_x - half_x, chip_y * GRID_X + chip_x))
    exp_chip = np.arange(EXPERTS) // (CORES * EXP_DEV)
    counts = BASE_ROWS + HOT_ROWS * (exp_chip[None, :] == dst_chip[:, None]).astype(np.int64)
    return np.stack([np.repeat(np.arange(EXPERTS), counts[row_id]) for row_id in range(GROUP_DEVS)]).astype(np.int32)


def slot_order(slot_key):
    return jax.random.permutation(slot_key, TOP_K)


def draw_routing(route_key):
    copy_table = jnp.asarray(sorted_lists())
    n_copy = TOK_DEV * TOP_K

    def one_device(dev_key, sorted_row):
        roll_key, tok_key, slot_key = jax.random.split(dev_key, 3)
        roll_by = jax.random.randint(roll_key, (), 0, n_copy)
        rolled = sorted_row[(jnp.arange(n_copy) + roll_by) % n_copy]
        layout = rolled.reshape(TOP_K, TOK_DEV).T
        layout = layout[jax.random.permutation(tok_key, TOK_DEV)]
        slot_perm = jax.vmap(slot_order)(jax.random.split(slot_key, TOK_DEV))
        return jnp.take_along_axis(layout, slot_perm, axis=1)

    ids_dev = jax.vmap(one_device)(jax.random.split(route_key, GROUP_DEVS), copy_table)
    return ids_dev.reshape(GROUP_DEVS * TOK_DEV, TOP_K)


def setup_inputs(seed: int = 0, part: int = 0) -> dict:
    base_key = jax.random.key(seed)
    weight_root, part_root = jax.random.split(base_key)
    part_key = jax.random.fold_in(part_root, part)
    tok_key, route_key, gate_key = jax.random.split(part_key, 3)
    wkey_gate, wkey_up, wkey_down = jax.random.split(weight_root, 3)
    n_tok = GROUP_DEVS * TOK_DEV
    tokens = jax.random.normal(tok_key, (n_tok, D_MODEL), jnp.float32).astype(jnp.bfloat16)
    expert_ids = draw_routing(route_key)
    gate_prob = jax.nn.softmax(0.5 * jax.random.normal(gate_key, (n_tok, TOP_K), jnp.float32), axis=-1)
    w_gate = (jax.random.normal(wkey_gate, (EXPERTS, D_MODEL, D_FF), jnp.float32) * D_MODEL ** -0.5).astype(jnp.bfloat16)
    w_up = (jax.random.normal(wkey_up, (EXPERTS, D_MODEL, D_FF), jnp.float32) * D_MODEL ** -0.5).astype(jnp.bfloat16)
    w_down = (jax.random.normal(wkey_down, (EXPERTS, D_FF, D_MODEL), jnp.float32) * D_FF ** -0.5).astype(jnp.bfloat16)
    return {'tokens': tokens, 'expert_ids': expert_ids, 'gate_prob': gate_prob, 'w_gate': w_gate, 'w_up': w_up, 'w_down': w_down}


def one_expert(packed):
    rows_in, wg_exp, wu_exp, wd_exp = packed
    gate_act = jnp.dot(rows_in, wg_exp, preferred_element_type=jnp.float32)
    up_act = jnp.dot(rows_in, wu_exp, preferred_element_type=jnp.float32)
    hidden = (jax.nn.silu(gate_act) * up_act).astype(jnp.bfloat16)
    return jnp.dot(hidden, wd_exp, preferred_element_type=jnp.float32).astype(jnp.bfloat16)


def reference(tokens, expert_ids, gate_prob, w_gate, w_up, w_down):
    n_tok = tokens.shape[0]
    n_copy = n_tok * TOP_K
    per_expert = n_copy // EXPERTS
    sort_order = jnp.argsort(expert_ids.reshape(n_copy), stable=True)
    grouped = tokens[sort_order // TOP_K].reshape(EXPERTS, per_expert, D_MODEL)
    y_grouped = lax.map(one_expert, (grouped, w_gate, w_up, w_down))
    y_copy = y_grouped.reshape(n_copy, D_MODEL)[jnp.argsort(sort_order)]
    y_copy = y_copy.reshape(n_tok, TOP_K, D_MODEL).astype(jnp.float32)
    mixed_out = jnp.sum(y_copy * gate_prob[:, :, None], axis=1)
    return mixed_out.astype(jnp.bfloat16)
```

```python
import functools

import jax
import jax.numpy as jnp
from jax import lax
from jax.experimental import pallas as pl
from jax.experimental.pallas import tpu as pltpu
from jax.sharding import PartitionSpec as P

GROUP_AXES = ('ey', 'ex', 'core')
CHIP_AXES = ('ey', 'ex')
TOKEN_SPEC = P(('dp', 'ey', 'ex', 'core'), None)
EXPERT_SPEC = P(('ey', 'ex', 'core'), None, None)
F32 = jnp.float32
BF16 = jnp.bfloat16
VMEM_LIMIT = 60 * 1024 * 1024


def target_chips(grid_y, grid_x):
    half_y, half_x = grid_y // 2, grid_x // 2
    chip_list = []
    for chip_y in range(grid_y):
        for chip_x in range(grid_x):
            if chip_y == 0 and chip_x < half_x:
                chip_list.append(half_y * grid_x + chip_x + half_x)
            elif chip_y == half_y and chip_x >= half_x:
                chip_list.append(chip_x - half_x)
            else:
                chip_list.append(chip_y * grid_x + chip_x)
    return chip_list


def row_to_columns(row):
    return jnp.transpose(jnp.broadcast_to(row, (128, row.shape[1])))


def pick_matrix(row, n_tok, first=0):
    cols = row_to_columns(row)
    lane = lax.broadcasted_iota(jnp.int32, cols.shape, 1)
    blocks = [(cols == lane + (first + 128 * k)).astype(F32).astype(BF16) for k in range(n_tok // 128)]
    return jnp.concatenate(blocks, axis=1)


def spread_matrix(row, n_tok):
    tok = lax.broadcasted_iota(jnp.int32, (n_tok, row.shape[1]), 0)
    return (tok == row).astype(F32).astype(BF16)


def scaled_rows(rows, gate_row):
    cols = row_to_columns(gate_row)
    reps = rows.shape[1] // 128
    return (rows.astype(F32) * jnp.concatenate([cols] * reps, axis=1)).astype(BF16)


def dot(a, b):
    return jnp.dot(a, b, preferred_element_type=F32)


def pick_kernel(slot_ref, idx_ref, own_ref, prev_ref, next_ref, far_lo_ref, far_hi_ref, out_ref):
    n_dst, _, base_rows, width = out_ref.shape
    tok_dev = own_ref.shape[0]
    half = tok_dev // 2
    for off, srcs in enumerate(((own_ref,), (prev_ref,), (far_lo_ref, far_hi_ref), (next_ref,))):
        slot = slot_ref[off]
        row = idx_ref[slot]
        if len(srcs) == 1:
            rows = dot(pick_matrix(row, tok_dev), srcs[0][...])
        else:
            rows = dot(pick_matrix(row, half), srcs[0][...]) + dot(pick_matrix(row, half, half), srcs[1][...])
        out_ref[:, pl.ds(slot, 1)] = rows.astype(BF16).reshape(n_dst, 1, base_rows, width)


def pick_rows(slots, idx, parts, n_dst, base_rows):
    width = parts[0].shape[1]
    n_src = idx.shape[0]
    n_row = n_dst * base_rows
    vm = pl.BlockSpec(memory_space=pltpu.VMEM)
    return pl.pallas_call(
        pick_kernel,
        out_shape=jax.ShapeDtypeStruct((n_dst, n_src, base_rows, width), BF16),
        in_specs=[pl.BlockSpec(memory_space=pltpu.SMEM)] + [vm] * 6,
        out_specs=vm,
        compiler_params=pltpu.CompilerParams(vmem_limit_bytes=VMEM_LIMIT),
        cost_estimate=pl.CostEstimate(flops=2 * n_src * n_row * parts[0].shape[0] * width, bytes_accessed=8 * n_src * n_row * width, transcendentals=0),
        name='pick_rows',
    )(slots, idx, *parts)


def hot_pick_kernel(sel_ref, idx_ref, own_ref, l1, h1, l2, h2, keep_ref, send_ref):
    exp_dev, hot_rows, d_model = keep_ref.shape
    tok_dev = own_ref.shape[0]
    half = tok_dev // 2
    dh = d_model // 2
    moved = sel_ref[0]
    core = sel_ref[1]
    for rel, out_ref in enumerate((keep_ref, send_ref)):
        for e in range(exp_dev):
            row = idx_ref[lax.rem(core + rel, 2) * exp_dev + e]

            @pl.when(moved == 0)
            def _():
                out_ref[e] = dot(pick_matrix(row, tok_dev), own_ref[...]).astype(BF16)

            @pl.when(moved != 0)
            def _():
                lo = pick_matrix(row, half)
                hi = pick_matrix(row, half, half)
                out_ref[e, :, :dh] = (dot(lo, l1[...]) + dot(hi, h1[...])).astype(BF16)
                out_ref[e, :, dh:] = (dot(lo, l2[...]) + dot(hi, h2[...])).astype(BF16)


def hot_pick(sel, idx, parts, exp_dev, hot_rows):
    tok_dev, d_model = parts[0].shape
    vm = pl.BlockSpec(memory_space=pltpu.VMEM)
    shape = jax.ShapeDtypeStruct((exp_dev, hot_rows, d_model), BF16)
    return pl.pallas_call(
        hot_pick_kernel,
        out_shape=(shape, shape),
        in_specs=[pl.BlockSpec(memory_space=pltpu.SMEM)] + [vm] * 6,
        out_specs=(vm, vm),
        compiler_params=pltpu.CompilerParams(vmem_limit_bytes=VMEM_LIMIT),
        cost_estimate=pl.CostEstimate(flops=4 * exp_dev * hot_rows * tok_dev * d_model, bytes_accessed=8 * exp_dev * hot_rows * d_model, transcendentals=0),
        name='hot_pick',
    )(sel, idx, *parts)


def gated_mlp(x, wg_ref, wu_ref, wd_ref):
    gate = dot(x, wg_ref[0])
    up = dot(x, wu_ref[0])
    hidden = (jax.nn.silu(gate) * up).astype(BF16)
    return dot(hidden, wd_ref[0]).astype(BF16)


def base_ffn_kernel(x1_ref, x2_ref, wg_ref, wu_ref, wd_ref, y1_ref, y2_ref):
    dh = x1_ref.shape[-1]
    n_core, n_col = x1_ref.shape[1], x1_ref.shape[2]
    base_rows = x1_ref.shape[3]
    for c in range(n_core):
        x1 = x1_ref[0, c].reshape(n_col * base_rows, dh)
        x2 = x2_ref[:, c, 0].reshape(n_col * base_rows, dh)
        gate = dot(x1, wg_ref[0, :dh]) + dot(x2, wg_ref[0, dh:])
        up = dot(x1, wu_ref[0, :dh]) + dot(x2, wu_ref[0, dh:])
        hidden = (jax.nn.silu(gate) * up).astype(BF16)
        y1_ref[0, c] = dot(hidden, wd_ref[0, :, :dh]).astype(BF16).reshape(n_col, base_rows, dh)
        y2_ref[:, c, 0] = dot(hidden, wd_ref[0, :, dh:]).astype(BF16).reshape(n_col, base_rows, dh)


def base_ffn(e, x1, x2, w_gate, w_up, w_down):
    grid_y, n_core, grid_x, base_rows, dh = x1.shape
    _, d_model, d_ff = w_gate.shape
    s1 = pl.BlockSpec((1, n_core, grid_x, base_rows, dh), lambda i: (i, 0, 0, 0, 0))
    s2 = pl.BlockSpec((grid_x, n_core, 1, base_rows, dh), lambda i: (0, 0, i, 0, 0))
    ws = pl.BlockSpec((1, d_model, d_ff), lambda i: (e, 0, 0))
    wd = pl.BlockSpec((1, d_ff, d_model), lambda i: (e, 0, 0))
    n_row = grid_y * n_core * grid_x * base_rows
    return pl.pallas_call(
        base_ffn_kernel,
        grid=(grid_y,),
        out_shape=(jax.ShapeDtypeStruct(x1.shape, BF16), jax.ShapeDtypeStruct(x2.shape, BF16)),
        in_specs=[s1, s2, ws, ws, wd],
        out_specs=(s1, s2),
        compiler_params=pltpu.CompilerParams(vmem_limit_bytes=VMEM_LIMIT),
        cost_estimate=pl.CostEstimate(flops=6 * n_row * d_model * d_ff, bytes_accessed=8 * n_row * d_model, transcendentals=n_row * d_ff),
        name='base_ffn',
    )(x1, x2, w_gate, w_up, w_down)


def hot_ffn_kernel(xa_ref, xb_ref, wg_ref, wu_ref, wd_ref, ya_ref, yb_ref):
    ya_ref[0] = gated_mlp(xa_ref[0], wg_ref, wu_ref, wd_ref)
    yb_ref[0] = gated_mlp(xb_ref[0], wg_ref, wu_ref, wd_ref)


def hot_ffn(xa, xb, w_gate, w_up, w_down):
    exp_dev, d_model, d_ff = w_gate.shape
    rows = xa.shape[1]
    spec = pl.BlockSpec((1, rows, d_model), lambda e: (e, 0, 0))
    ws = pl.BlockSpec((1, d_model, d_ff), lambda e: (e, 0, 0))
    wd = pl.BlockSpec((1, d_ff, d_model), lambda e: (e, 0, 0))
    n_row = 2 * exp_dev * rows
    return pl.pallas_call(
        hot_ffn_kernel,
        grid=(exp_dev,),
        out_shape=(jax.ShapeDtypeStruct(xa.shape, BF16),) * 2,
        in_specs=[spec, spec, ws, ws, wd],
        out_specs=(spec, spec),
        compiler_params=pltpu.CompilerParams(vmem_limit_bytes=VMEM_LIMIT),
        cost_estimate=pl.CostEstimate(flops=6 * n_row * d_model * d_ff, bytes_accessed=8 * n_row * d_model, transcendentals=n_row * d_ff),
        name='hot_ffn',
    )(xa, xb, w_gate, w_up, w_down)


def spread_kernel(slot_ref, idx0_ref, idx1_ref, g0_ref, g1_ref, r0_ref, r1_ref, *out_refs):
    n_dst, _, base_rows, width = r0_ref.shape
    tok_dev = out_refs[0].shape[0]
    half = tok_dev // 2
    own, prev_lo, prev_hi, far_lo, far_hi, next_lo, next_hi = out_refs
    for off, outs in enumerate(((own,), (prev_lo, prev_hi), (far_lo, far_hi), (next_lo, next_hi))):
        slot = slot_ref[off]
        acc = None
        for idx_ref, g_ref, r_ref in ((idx0_ref, g0_ref, r0_ref), (idx1_ref, g1_ref, r1_ref)):
            rows = r_ref[:, pl.ds(slot, 1)].reshape(n_dst * base_rows, width)
            part = dot(spread_matrix(idx_ref[slot], tok_dev), scaled_rows(rows, g_ref[slot]))
            acc = part if acc is None else acc + part
        acc = acc.astype(BF16)
        if len(outs) == 1:
            outs[0][...] = acc
        else:
            outs[0][...] = acc[:half]
            outs[1][...] = acc[half:]


def spread_rows(slots, idx, gate, ret, tok_dev):
    n_dst, n_src, base_rows, width = ret[0].shape
    vm = pl.BlockSpec(memory_space=pltpu.VMEM)
    full = jax.ShapeDtypeStruct((tok_dev, width), BF16)
    part = jax.ShapeDtypeStruct((tok_dev // 2, width), BF16)
    n_row = 2 * n_dst * base_rows
    return pl.pallas_call(
        spread_kernel,
        out_shape=(full,) + (part,) * 6,
        in_specs=[pl.BlockSpec(memory_space=pltpu.SMEM)] + [vm] * 6,
        out_specs=(vm,) * 7,
        compiler_params=pltpu.CompilerParams(vmem_limit_bytes=VMEM_LIMIT),
        cost_estimate=pl.CostEstimate(flops=2 * n_src * n_row * tok_dev * width, bytes_accessed=4 * n_src * n_row * width, transcendentals=0),
        name='spread_rows',
    )(slots, idx[0], idx[1], gate[0], gate[1], ret[0], ret[1])


def hot_spread_kernel(sel_ref, idx_ref, g_ref, keep_ref, back_ref, s1l, s1h, s2l, s2h):
    exp_dev, hot_rows, d_model = keep_ref.shape
    half = s1l.shape[0]
    dh = d_model // 2
    core = sel_ref[1]
    for part, (lo, hi) in enumerate(((s1l, s1h), (s2l, s2h))):
        acc = None
        for rel, r_ref in enumerate((keep_ref, back_ref)):
            for e in range(exp_dev):
                k = lax.rem(core + rel, 2) * exp_dev + e
                rows = scaled_rows(r_ref[e, :, part * dh:(part + 1) * dh], g_ref[k])
                term = dot(spread_matrix(idx_ref[k], 2 * half), rows)
                acc = term if acc is None else acc + term
        acc = acc.astype(BF16)
        lo[...] = acc[:half]
        hi[...] = acc[half:]


def hot_spread(sel, idx, gate, keep, back, tok_dev):
    exp_dev, hot_rows, d_model = keep.shape
    vm = pl.BlockSpec(memory_space=pltpu.VMEM)
    part = jax.ShapeDtypeStruct((tok_dev // 2, d_model // 2), BF16)
    return pl.pallas_call(
        hot_spread_kernel,
        out_shape=(part,) * 4,
        in_specs=[pl.BlockSpec(memory_space=pltpu.SMEM)] + [vm] * 4,
        out_specs=(vm,) * 4,
        compiler_params=pltpu.CompilerParams(vmem_limit_bytes=VMEM_LIMIT),
        cost_estimate=pl.CostEstimate(flops=4 * exp_dev * hot_rows * tok_dev * d_model, bytes_accessed=4 * exp_dev * hot_rows * d_model, transcendentals=0),
        name='hot_spread',
    )(sel, idx, gate, keep, back)


def final_kernel(sel_ref, p1, w1l, w1h, z1l, z1h, p2, w2l, w2h, z2l, z2h, s1l, s1h, s2l, s2h, out_ref):
    half, dh = s1l.shape
    keep = jnp.where(sel_ref[0] == 0, 1.0, 0.0).astype(F32)
    for k, (p, w, z, s) in enumerate(((p1, (w1l, w1h), (z1l, z1h), (s1l, s1h)), (p2, (w2l, w2h), (z2l, z2h), (s2l, s2h)))):
        for r in range(2):
            rows = pl.ds(r * half, half)
            acc = p[rows].astype(F32) + w[r][...].astype(F32) + z[r][...].astype(F32)
            out_ref[rows, k * dh:(k + 1) * dh] = (acc + keep * s[r][...].astype(F32)).astype(BF16)


def final_sum(sel, args, tok_dev, d_model):
    vm = pl.BlockSpec(memory_space=pltpu.VMEM)
    return pl.pallas_call(
        final_kernel,
        out_shape=jax.ShapeDtypeStruct((tok_dev, d_model), BF16),
        in_specs=[pl.BlockSpec(memory_space=pltpu.SMEM)] + [vm] * 14,
        out_specs=vm,
        compiler_params=pltpu.CompilerParams(vmem_limit_bytes=VMEM_LIMIT),
        name='final_sum',
    )(sel, *args)


def solution(mesh):
    grid_y = mesh.shape['ey']
    grid_x = mesh.shape['ex']
    n_core = mesh.shape['core']
    n_dev = grid_y * grid_x * n_core
    chip_list = target_chips(grid_y, grid_x)
    sizes = {'ey': grid_y, 'ex': grid_x}

    def shift(x, axis, by):
        n = sizes[axis]
        return lax.ppermute(x, axis, [(i, (i + by) % n) for i in range(n)])

    moved_chips = [k for k in range(grid_y * grid_x) if chip_list[k] != k]

    def hot_pairs(first_axis):
        pairs = []
        for k in moved_chips:
            dst = chip_list[k]
            if first_axis == 'ex':
                mid = (k // grid_x) * grid_x + dst % grid_x
            else:
                mid = (dst // grid_x) * grid_x + k % grid_x
            pairs += [(mid * n_core + c, dst * n_core + c) for c in range(n_core)]
        return pairs

    def back(pairs):
        return [(b, a) for a, b in pairs]

    def device_body(tokens, expert_ids, gate_prob, w_gate, w_up, w_down):
        tok_dev, top_k = expert_ids.shape
        d_model = tokens.shape[1]
        dh = d_model // 2
        half = tok_dev // 2
        exp_dev = w_gate.shape[0]
        exp_chip = exp_dev * n_core
        n_exp = exp_dev * n_dev
        n_copy = tok_dev * top_k
        base_rows = 2 * n_copy // (3 * n_exp)
        hot_rows = grid_y * grid_x * base_rows // 2
        n_base = n_exp * base_rows
        core = lax.axis_index('core')
        iy = lax.axis_index('ey')
        ix = lax.axis_index('ex')
        chip = iy * grid_x + ix
        dst_chip = jnp.asarray(chip_list, dtype=jnp.int32)[chip]
        sel = jnp.stack([(dst_chip != chip).astype(jnp.int32), core.astype(jnp.int32)])

        def ring_gather(x, axis):
            prev = shift(x, axis, 1)
            nxt = shift(x, axis, -1)
            far_lo = shift(prev[:half], axis, 1)
            far_hi = shift(nxt[half:], axis, -1)
            return x, prev, nxt, far_lo, far_hi

        parts1 = ring_gather(tokens[:, :dh], 'ex')
        parts2 = ring_gather(tokens[:, dh:], 'ey')

        key = expert_ids.reshape(n_copy) * n_copy + jnp.arange(n_copy, dtype=jnp.int32)
        skey, sgate = lax.sort((key, gate_prob.reshape(n_copy)), num_keys=1, is_stable=False)
        stok = (lax.rem(skey, n_copy) // top_k).astype(F32)
        tab = jnp.stack([stok, sgate])
        lo = dst_chip * exp_chip
        hot_shift = hot_rows * exp_chip // base_rows
        by_block = tab.reshape(2, n_copy // base_rows, base_rows)
        e_id = jnp.arange(n_exp)[None, :, None]
        base = jnp.where(e_id < lo, by_block[:, :n_exp], by_block[:, hot_shift:hot_shift + n_exp])
        hot = lax.dynamic_slice(tab, (0, lo * base_rows), (2, exp_chip * (base_rows + hot_rows)))
        hot = hot.reshape(2, exp_chip, base_rows + hot_rows)
        base = lax.dynamic_update_slice(base, hot[:, :, :base_rows], (0, lo, 0))
        tab = jnp.concatenate([base.reshape(2, n_base), hot[:, :, base_rows:].reshape(2, -1)], axis=1)
        tabs = lax.all_gather(tab, CHIP_AXES).reshape(grid_y, grid_x, 2, n_copy)

        row_tab = lax.dynamic_index_in_dim(tabs, iy, 0, keepdims=False)[:, :, :n_base]
        row_tab = row_tab.reshape(grid_x, 2, grid_y, grid_x, n_core, exp_dev, base_rows)
        row_tab = lax.dynamic_index_in_dim(row_tab, ix, 3, keepdims=False)
        col_tab = lax.dynamic_index_in_dim(tabs, ix, 1, keepdims=False)[:, :, :n_base]
        col_tab = col_tab.reshape(grid_y, 2, grid_y, grid_x, n_core, exp_dev, base_rows)
        col_tab = lax.dynamic_index_in_dim(col_tab, iy, 2, keepdims=False)
        hot_tab = lax.dynamic_index_in_dim(tabs.reshape(grid_y * grid_x, 2, n_copy), dst_chip, 0, keepdims=False)
        hot_tab = hot_tab[:, n_base:].reshape(2, exp_chip, 1, hot_rows)
        hot_idx = hot_tab[0].astype(jnp.int32)
        hot_gate = hot_tab[1]

        def split_tab(t, e):
            rows = t[:, :, :, :, e].reshape(t.shape[0], 2, 1, -1)
            return rows[:, 0].astype(jnp.int32), rows[:, 1]

        tab1 = [split_tab(row_tab, e) for e in range(exp_dev)]
        tab2 = [split_tab(col_tab, e) for e in range(exp_dev)]

        def slot_list(me, n):
            return jnp.stack([lax.rem(me - off + n, n) for off in range(n)]).astype(jnp.int32)

        slots1 = slot_list(ix, grid_x)
        slots2 = slot_list(iy, grid_y)

        pairs1 = hot_pairs('ex')
        pairs2 = hot_pairs('ey')
        hot_in = [lax.ppermute(p, GROUP_AXES, pr) for p, pr in ((parts1[3], pairs1), (parts1[4], pairs1), (parts2[3], pairs2), (parts2[4], pairs2))]

        recv = []
        for e in range(exp_dev):
            g1 = pick_rows(slots1, tab1[e][0], parts1, grid_y * n_core, base_rows)
            g2 = pick_rows(slots2, tab2[e][0], parts2, grid_x * n_core, base_rows)
            r1 = lax.all_to_all(g1, ('ey', 'core'), 0, 0, tiled=True)
            r2 = lax.all_to_all(g2, ('ex', 'core'), 0, 0, tiled=True)
            recv.append((r1.reshape(grid_y, n_core, grid_x, base_rows, dh), r2.reshape(grid_x, n_core, grid_y, base_rows, dh)))

        swap = [(c, (c + 1) % n_core) for c in range(n_core)]
        hot_keep, hot_send = hot_pick(sel, hot_idx, [tokens] + hot_in, exp_dev, hot_rows)
        hot_recv = lax.ppermute(hot_send, 'core', swap)

        ret1, ret2 = [], []
        for e in range(exp_dev):
            y1, y2 = base_ffn(e, recv[e][0], recv[e][1], w_gate, w_up, w_down)
            y1 = y1.reshape(grid_y * n_core, grid_x, base_rows, dh)
            y2 = y2.reshape(grid_x * n_core, grid_y, base_rows, dh)
            ret1.append(lax.all_to_all(y1, ('ey', 'core'), 0, 0, tiled=True))
            ret2.append(lax.all_to_all(y2, ('ex', 'core'), 0, 0, tiled=True))

        y_keep, y_send = hot_ffn(hot_keep, hot_recv, w_gate, w_up, w_down)
        y_back = lax.ppermute(y_send, 'core', swap)
        s_parts = hot_spread(sel, hot_idx, hot_gate, y_keep, y_back, tok_dev)
        hot_out = [lax.ppermute(s, GROUP_AXES, back(pr)) for s, pr in zip(s_parts, (pairs1, pairs1, pairs2, pairs2))]

        def add(a, b):
            return (a.astype(F32) + b.astype(F32)).astype(BF16)

        def ring_scatter(slots, tabs_e, ret, axis, hot_lo, hot_hi):
            own, prev_lo, prev_hi, far_lo, far_hi, next_lo, next_hi = spread_rows(
                slots, [t[0] for t in tabs_e], [t[1] for t in tabs_e], ret, tok_dev)
            up = shift(add(far_lo, hot_lo), axis, 1)
            down = shift(add(far_hi, hot_hi), axis, -1)
            w_hi = shift(next_hi, axis, 1)
            z_lo = shift(prev_lo, axis, -1)
            w_lo = shift(add(next_lo, up), axis, 1)
            z_hi = shift(add(prev_hi, down), axis, -1)
            return own, w_lo, w_hi, z_lo, z_hi

        out1 = ring_scatter(slots1, tab1, ret1, 'ex', hot_out[0], hot_out[1])
        out2 = ring_scatter(slots2, tab2, ret2, 'ey', hot_out[2], hot_out[3])
        return final_sum(sel, list(out1) + list(out2) + list(s_parts), tok_dev, d_model)

    return jax.shard_map(device_body, mesh=mesh, in_specs=(TOKEN_SPEC, TOKEN_SPEC, TOKEN_SPEC, EXPERT_SPEC, EXPERT_SPEC, EXPERT_SPEC), out_specs=TOKEN_SPEC, check_vma=False)
```

```python
import functools

import jax
import jax.numpy as jnp
from jax import lax
from jax.experimental import pallas as pl
from jax.experimental.pallas import tpu as pltpu
from jax.sharding import PartitionSpec as P

TOKEN_SPEC = P(('dp', 'ey', 'ex', 'core'), None)
EXPERT_SPEC = P(('ey', 'ex', 'core'), None, None)
F32 = jnp.float32
BF16 = jnp.bfloat16
VMEM_LIMIT = 62 * 1024 * 1024
MESH = pl.DeviceIdType.MESH
AXES = (('ex', 'ey'), ('ey', 'ex'))


def target_chips(grid_y, grid_x):
    half_y, half_x = grid_y // 2, grid_x // 2
    chip_list = []
    for chip_y in range(grid_y):
        for chip_x in range(grid_x):
            if chip_y == 0 and chip_x < half_x:
                chip_list.append(half_y * grid_x + chip_x + half_x)
            elif chip_y == half_y and chip_x >= half_x:
                chip_list.append(chip_x - half_x)
            else:
                chip_list.append(chip_y * grid_x + chip_x)
    return chip_list


def is_moved(iy, ix, n):
    half = n // 2
    return ((iy == 0) & (ix < half)) | ((iy == half) & (ix >= half))


def row_to_columns(row):
    return jnp.transpose(jnp.broadcast_to(row, (128, row.shape[1])))


def pick_matrix(row, n_tok):
    cols = row_to_columns(row)
    lane = lax.broadcasted_iota(jnp.int32, cols.shape, 1).astype(F32)
    blocks = [(cols == lane + (128.0 * k)).astype(F32).astype(BF16) for k in range(n_tok // 128)]
    return jnp.concatenate(blocks, axis=1)


def spread_matrix(row, n_tok):
    tok = lax.broadcasted_iota(jnp.int32, (n_tok, row.shape[1]), 0).astype(F32)
    return (tok == row).astype(F32).astype(BF16)


def scaled_rows(rows, gate_row):
    cols = row_to_columns(gate_row)
    reps = rows.shape[1] // 128
    return (rows.astype(F32) * jnp.concatenate([cols] * reps, axis=1)).astype(BF16)


def dot(a, b):
    return jnp.dot(a, b, preferred_element_type=F32)


class Here:
    def __init__(self, n, n_core):
        self.n, self.n_core = n, n_core
        self.iy, self.ix, self.ic = (lax.axis_index(a) for a in ('ey', 'ex', 'core'))
        self.at = {'ey': self.iy, 'ex': self.ix, 'core': self.ic}

    def step(self, axis, by):
        size = self.n_core if axis == 'core' else self.n
        return lax.rem(self.at[axis] + (by % size), size)

    def dev(self, **by):
        return {axis: self.step(axis, k) for axis, k in by.items()}

    def moved(self):
        return is_moved(self.iy, self.ix, self.n)

    def middle(self):
        return is_moved(self.iy, self.step('ex', self.n // 2), self.n)

    def barrier(self):
        sem = pltpu.get_barrier_semaphore()
        peers = [self.dev(**{axis: k, 'core': c}) for axis in ('ey', 'ex') for k in range(1, self.n) for c in range(self.n_core)]
        peers += [self.dev(core=1), self.dev(ey=self.n // 2, ex=self.n // 2)]
        for peer in peers:
            pl.semaphore_signal(sem, inc=1, device_id=peer, device_id_type=MESH)
        pl.semaphore_wait(sem, len(peers))


def remote(src, dst, send_sem, recv_sem, dev):
    return pltpu.make_async_remote_copy(src_ref=src, dst_ref=dst, send_sem=send_sem, recv_sem=recv_sem, device_id=dev, device_id_type=MESH)


def dispatch_kernel(n, n_core, tok_ref, tx_ref, ht_ref, rx_ref, htr_ref, r1_ref, r2_ref, hk_ref, hr_ref,
                    g_ref, hb_ref, sb_ref, hp_ref, own_sem, tab_s, tab_r, g_s, g_r, d_s, d_r, hot_s, hot_r, swap_s, swap_r, keep_sem):
    here = Here(n, n_core)
    tok_dev, d_model = tok_ref.shape
    dh = d_model // 2
    half = tok_dev // 2
    lo, hi = pl.ds(0, half), pl.ds(half, half)
    n_dst, n_src, base_rows, _ = sb_ref.shape[2:]
    exp_dev = sb_ref.shape[1]
    outs = (r1_ref, r2_ref)
    own = [pltpu.make_async_copy(tok_ref.at[:, pl.ds(h * dh, dh)], g_ref.at[h, 0], own_sem.at[h]) for h in range(2)]
    for c in own:
        c.start()
    here.barrier()

    tabs = []
    for h in range(2):
        rx_ref[h, 0] = tx_ref[h, 0]
        for k in range(1, n):
            c = remote(tx_ref.at[h, k], rx_ref.at[h, k], tab_s.at[h * n + k], tab_r.at[h * n + k], here.dev(**{AXES[h][0]: k}))
            c.start()
            tabs.append(c)
    moved = here.moved()
    middle = here.middle()
    hot_tab = remote(ht_ref, htr_ref, tab_s.at[0], tab_r.at[0], here.dev(ey=n // 2, ex=n // 2))

    @pl.when(moved)
    def _():
        hot_tab.start()

    @pl.when(jnp.logical_not(moved))
    def _():
        htr_ref[...] = ht_ref[...]

    first = []
    for h in range(2):
        own[h].wait()
        axis = AXES[h][0]
        for i, (slot, rows, by) in enumerate(((1, lo, 1), (3, hi, -1), (1, hi, 1), (3, lo, -1))):
            c = remote(g_ref.at[h, 0, rows], g_ref.at[h, slot, rows], g_s.at[h, i], g_r.at[h, i], here.dev(**{axis: by}))
            c.start()
            first.append(c)
    far = []
    for i, (slot, rows, by) in enumerate(((1, lo, 1), (3, hi, -1))):
        for h in range(2):
            first[h * 4 + i].wait_recv()
            c = remote(g_ref.at[h, slot, rows], g_ref.at[h, 2, rows], g_s.at[h, 4 + i], g_r.at[h, 4 + i], here.dev(**{AXES[h][0]: by}))
            c.start()
            far.append(c)
    for c in tabs:
        c.wait_recv()

    for h in range(2):
        first[h * 4 + 2].wait_recv()
        first[h * 4 + 3].wait_recv()
    for c in far:
        c.wait_recv()
    sends = []
    for e in range(exp_dev):
        for h in range(2):
            @pl.loop(0, n_src)
            def _(s):
                mat = pick_matrix(rx_ref[h, s, 2 * e:2 * e + 1], tok_dev)
                sb_ref[h, e, :, pl.ds(s, 1)] = dot(mat, g_ref[h, s]).astype(BF16).reshape(n_dst, 1, base_rows, dh)

            for j in range(n_dst - 1, 0, -1):
                c = remote(sb_ref.at[h, e, j], outs[h].at[e, j], d_s.at[h, e, j], d_r.at[h, e, j], here.dev(**{AXES[h][1]: j // n_core, 'core': j % n_core}))
                c.start()
                sends.append(c)
            c = pltpu.make_async_copy(sb_ref.at[h, e, 0], outs[h].at[e, 0], d_s.at[h, e, 0])
            c.start()
            sends.append(c)

    hot = [remote(g_ref.at[h, 2], hb_ref.at[h], hot_s.at[h], hot_r.at[h], here.dev(**{AXES[h][1]: n // 2})) for h in range(2)]

    @pl.when(middle)
    def _():
        for c in hot:
            c.start()

    @pl.when(jnp.logical_not(moved))
    def _():
        for h in range(2):
            hb_ref[h] = g_ref[h, 0]

    @pl.when(moved)
    def _():
        hot_tab.wait_recv()
        for c in hot:
            c.wait_recv()

    swap = []
    for rel in range(n_core - 1, -1, -1):
        @pl.loop(0, exp_dev)
        def _(e):
            mat = pick_matrix(htr_ref[pl.ds(rel * exp_dev + e, 1)], tok_dev)
            for h in range(2):
                hp_ref[rel, e, :, h * dh:(h + 1) * dh] = dot(mat, hb_ref[h]).astype(BF16)

        if rel:
            c = remote(hp_ref.at[rel], hr_ref, swap_s, swap_r, here.dev(core=rel))
        else:
            c = pltpu.make_async_copy(hp_ref.at[rel], hk_ref, keep_sem)
        c.start()
        swap.append(c)

    for c in swap + sends + tabs:
        c.wait() if not c.is_remote else c.wait_send()
    for c in first + far:
        c.wait_send()
    for c in sends:
        if c.is_remote:
            c.wait_recv()
    swap[0].wait_recv()

    @pl.when(moved)
    def _():
        hot_tab.wait_send()

    @pl.when(middle)
    def _():
        for c in hot:
            c.wait_send()


def dispatch(n, n_core, exp_dev, base_rows, hot_rows, tokens, tx, ht):
    tok_dev, d_model = tokens.shape
    dh = d_model // 2
    n_dst = n * n_core
    any_ = pl.BlockSpec(memory_space=pl.ANY)
    vm = pl.BlockSpec(memory_space=pltpu.VMEM)
    recv = jax.ShapeDtypeStruct((exp_dev, n_dst, n, base_rows, dh), BF16)
    hot = jax.ShapeDtypeStruct((exp_dev, hot_rows, d_model), BF16)
    dma = pltpu.SemaphoreType.DMA
    return pl.pallas_call(
        functools.partial(dispatch_kernel, n, n_core),
        out_shape=(jax.ShapeDtypeStruct(tx.shape, F32), jax.ShapeDtypeStruct(ht.shape, F32), recv, recv, hot, hot),
        in_specs=[any_, vm, vm],
        out_specs=(vm, vm, any_, any_, any_, any_),
        scratch_shapes=[
            pltpu.VMEM((2, n, tok_dev, dh), BF16),
            pltpu.VMEM((2, tok_dev, dh), BF16),
            pltpu.VMEM((2, exp_dev, n_dst, n, base_rows, dh), BF16),
            pltpu.VMEM((n_core, exp_dev, hot_rows, d_model), BF16),
            dma((2,)), dma((2 * n,)), dma((2 * n,)), dma((2, 6)), dma((2, 6)),
            dma((2, exp_dev, n_dst)), dma((2, exp_dev, n_dst)), dma((2,)), dma((2,)), dma, dma, dma,
        ],
        compiler_params=pltpu.CompilerParams(vmem_limit_bytes=VMEM_LIMIT, collective_id=0, has_side_effects=True),
        name='dispatch',
    )(tokens, tx, ht)


def return_kernel(n, n_core, rx_ref, htr_ref, y1e0, y2e0, y1e1, y2e1, hk_ref, hr_ref, out_ref,
                  q_ref, hy_ref, p_ref, s_ref, hs_ref, u_ref, w_ref, d_s, d_r, swap_s, swap_r, keep_sem, hot_s, hot_r, ring_s, ring_r):
    here = Here(n, n_core)
    tok_dev, d_model = out_ref.shape
    dh = d_model // 2
    half = tok_dev // 2
    lo, hi = pl.ds(0, half), pl.ds(half, half)
    exp_dev, n_dst, n_src, base_rows, _ = q_ref.shape[1:]
    ys = ((y1e0, y1e1), (y2e0, y2e1))
    keep = pltpu.make_async_copy(hk_ref, hy_ref.at[0], keep_sem)
    keep.start()
    here.barrier()
    sends = []
    for e in range(exp_dev):
        for h in range(2):
            for j in range(n_dst - 1, 0, -1):
                c = remote(ys[h][e].at[j], q_ref.at[h, e, j], d_s.at[h, e, j], d_r.at[h, e, j], here.dev(**{AXES[h][1]: -(j // n_core), 'core': j % n_core}))
                c.start()
                sends.append(c)
            c = pltpu.make_async_copy(ys[h][e].at[0], q_ref.at[h, e, 0], d_s.at[h, e, 0])
            c.start()
            sends.append(c)
        if e == 0:
            swap = remote(hr_ref, hy_ref.at[1], swap_s, swap_r, here.dev(core=1))
            swap.start()
    moved = here.moved()
    middle = here.middle()

    keep.wait()
    swap.wait_recv()
    for h in range(2):
        acc = None
        for k in range(n_core * exp_dev):
            rows = scaled_rows(hy_ref[k // exp_dev, k % exp_dev, :, h * dh:(h + 1) * dh], htr_ref[n_core * exp_dev + k:n_core * exp_dev + k + 1])
            term = dot(spread_matrix(htr_ref[k:k + 1], tok_dev), rows)
            acc = term if acc is None else acc + term
        s_ref[h] = acc.astype(BF16)
    hot = [remote(s_ref.at[h], hs_ref.at[h], hot_s.at[h], hot_r.at[h], here.dev(**{AXES[h][1]: n // 2})) for h in range(2)]

    @pl.when(moved)
    def _():
        for c in hot:
            c.start()

    for c in sends:
        if c.is_remote:
            c.wait_recv()
        else:
            c.wait()

    @pl.when(middle)
    def _():
        for c in hot:
            c.wait_recv()

    def spread(h, s):
        acc = None
        for e in range(exp_dev):
            rows = q_ref[h, e, :, s].reshape(n_dst * base_rows, dh)
            term = dot(spread_matrix(rx_ref[h, s, 2 * e:2 * e + 1], tok_dev), scaled_rows(rows, rx_ref[h, s, 2 * e + 1:2 * e + 2]))
            acc = term if acc is None else acc + term
        return acc

    ring = []

    def send(h, i, src, dst, by):
        c = remote(src, dst, ring_s.at[h, i], ring_r.at[h, i], here.dev(**{AXES[h][0]: by}))
        c.start()
        ring.append(c)
        return c

    ups, downs = [], []
    for h in range(2):
        p_ref[h, 2] = spread(h, 2).astype(BF16)

        @pl.when(middle)
        def _():
            p_ref[h, 2] = (p_ref[h, 2].astype(F32) + hs_ref[h].astype(F32)).astype(BF16)

        ups.append(send(h, 0, p_ref.at[h, 2, lo], u_ref.at[h, lo], 1))
        downs.append(send(h, 1, p_ref.at[h, 2, hi], u_ref.at[h, hi], -1))
    last = []
    for h in range(2):
        p_ref[h, 3] = spread(h, 3).astype(BF16)
        last.append(send(h, 2, p_ref.at[h, 3, hi], w_ref.at[h, 0, hi], 1))
        p_ref[h, 1] = spread(h, 1).astype(BF16)
        last.append(send(h, 3, p_ref.at[h, 1, lo], w_ref.at[h, 1, lo], -1))
    for h in range(2):
        ups[h].wait_recv()
        p_ref[h, 3, lo] = (p_ref[h, 3, lo].astype(F32) + u_ref[h, lo].astype(F32)).astype(BF16)
        last.append(send(h, 4, p_ref.at[h, 3, lo], w_ref.at[h, 0, lo], 1))
        downs[h].wait_recv()
        p_ref[h, 1, hi] = (p_ref[h, 1, hi].astype(F32) + u_ref[h, hi].astype(F32)).astype(BF16)
        last.append(send(h, 5, p_ref.at[h, 1, hi], w_ref.at[h, 1, hi], -1))
    own_hot = jnp.where(moved, 0.0, 1.0).astype(F32)
    for h in range(2):
        p_ref[h, 0] = (spread(h, 0) + own_hot * s_ref[h].astype(F32)).astype(BF16)
    for c in last:
        c.wait_recv()
    for h in range(2):
        out_ref[:, h * dh:(h + 1) * dh] = (p_ref[h, 0].astype(F32) + w_ref[h, 0].astype(F32) + w_ref[h, 1].astype(F32)).astype(BF16)

    for c in sends:
        if c.is_remote:
            c.wait_send()
    swap.wait_send()
    for c in ring:
        c.wait_send()

    @pl.when(moved)
    def _():
        for c in hot:
            c.wait_send()


def combine(n, n_core, tok_dev, rx, htr, ys, hk, hr):
    exp_dev, n_dst, n_src, base_rows, dh = 2, *ys[0].shape
    any_ = pl.BlockSpec(memory_space=pl.ANY)
    vm = pl.BlockSpec(memory_space=pltpu.VMEM)
    dma = pltpu.SemaphoreType.DMA
    half_tok = pltpu.VMEM((2, tok_dev, dh), BF16)
    return pl.pallas_call(
        functools.partial(return_kernel, n, n_core),
        out_shape=jax.ShapeDtypeStruct((tok_dev, 2 * dh), BF16),
        in_specs=[vm, vm] + [any_] * 6,
        out_specs=vm,
        scratch_shapes=[
            pltpu.VMEM((2, exp_dev, n_dst, n_src, base_rows, dh), BF16),
            pltpu.VMEM((n_core,) + hk.shape, BF16),
            pltpu.VMEM((2, n, tok_dev, dh), BF16),
            half_tok, half_tok, half_tok,
            pltpu.VMEM((2, 2, tok_dev, dh), BF16),
            dma((2, exp_dev, n_dst)), dma((2, exp_dev, n_dst)), dma, dma, dma, dma((2,)), dma((2,)), dma((2, 6)), dma((2, 6)),
        ],
        compiler_params=pltpu.CompilerParams(vmem_limit_bytes=VMEM_LIMIT, collective_id=1, has_side_effects=True),
        name='combine',
    )(rx, htr, *ys, hk, hr)


def gated_mlp(x, wg_ref, wu_ref, wd_ref):
    gate = dot(x, wg_ref[0])
    up = dot(x, wu_ref[0])
    hidden = (jax.nn.silu(gate) * up).astype(BF16)
    return dot(hidden, wd_ref[0]).astype(BF16)


def base_ffn_kernel(x1_ref, x2_ref, wg_ref, wu_ref, wd_ref, y1_ref, y2_ref):
    dh = x1_ref.shape[-1]
    n_core, n_col, base_rows = x1_ref.shape[2:5]
    for c in range(n_core):
        x1 = x1_ref[0, 0, c].reshape(n_col * base_rows, dh)
        x2 = x2_ref[0, :, c, 0].reshape(n_col * base_rows, dh)
        gate = dot(x1, wg_ref[0, :dh]) + dot(x2, wg_ref[0, dh:])
        up = dot(x1, wu_ref[0, :dh]) + dot(x2, wu_ref[0, dh:])
        hidden = (jax.nn.silu(gate) * up).astype(BF16)
        y1_ref[0, c] = dot(hidden, wd_ref[0, :, :dh]).astype(BF16).reshape(n_col, base_rows, dh)
        y2_ref[:, c, 0] = dot(hidden, wd_ref[0, :, dh:]).astype(BF16).reshape(n_col, base_rows, dh)


def base_ffn(e, r1, r2, w_gate, w_up, w_down):
    _, n, n_core, _, base_rows, dh = r1.shape
    _, d_model, d_ff = w_gate.shape
    ws = pl.BlockSpec((1, d_model, d_ff), lambda i: (e, 0, 0))
    wd = pl.BlockSpec((1, d_ff, d_model), lambda i: (e, 0, 0))
    out = jax.ShapeDtypeStruct((n, n_core, n, base_rows, dh), BF16)
    n_row = n * n_core * n * base_rows
    return pl.pallas_call(
        base_ffn_kernel,
        grid=(n,),
        out_shape=(out, out),
        in_specs=[
            pl.BlockSpec((1, 1, n_core, n, base_rows, dh), lambda i: (e, i, 0, 0, 0, 0)),
            pl.BlockSpec((1, n, n_core, 1, base_rows, dh), lambda i: (e, 0, 0, i, 0, 0)),
            ws, ws, wd,
        ],
        out_specs=(
            pl.BlockSpec((1, n_core, n, base_rows, dh), lambda i: (i, 0, 0, 0, 0)),
            pl.BlockSpec((n, n_core, 1, base_rows, dh), lambda i: (0, 0, i, 0, 0)),
        ),
        compiler_params=pltpu.CompilerParams(vmem_limit_bytes=VMEM_LIMIT),
        cost_estimate=pl.CostEstimate(flops=6 * n_row * d_model * d_ff, bytes_accessed=8 * n_row * d_model, transcendentals=n_row * d_ff),
        name='base_ffn',
    )(r1, r2, w_gate, w_up, w_down)


def hot_ffn_kernel(xa_ref, xb_ref, wg_ref, wu_ref, wd_ref, ya_ref, yb_ref):
    ya_ref[0] = gated_mlp(xa_ref[0], wg_ref, wu_ref, wd_ref)
    yb_ref[0] = gated_mlp(xb_ref[0], wg_ref, wu_ref, wd_ref)


def hot_ffn(xa, xb, w_gate, w_up, w_down):
    exp_dev, d_model, d_ff = w_gate.shape
    rows = xa.shape[1]
    spec = pl.BlockSpec((1, rows, d_model), lambda e: (e, 0, 0))
    ws = pl.BlockSpec((1, d_model, d_ff), lambda e: (e, 0, 0))
    wd = pl.BlockSpec((1, d_ff, d_model), lambda e: (e, 0, 0))
    n_row = 2 * exp_dev * rows
    return pl.pallas_call(
        hot_ffn_kernel,
        grid=(exp_dev,),
        out_shape=(jax.ShapeDtypeStruct(xa.shape, BF16),) * 2,
        in_specs=[spec, spec, ws, ws, wd],
        out_specs=(spec, spec),
        compiler_params=pltpu.CompilerParams(vmem_limit_bytes=VMEM_LIMIT),
        cost_estimate=pl.CostEstimate(flops=6 * n_row * d_model * d_ff, bytes_accessed=8 * n_row * d_model, transcendentals=n_row * d_ff),
        name='hot_ffn',
    )(xa, xb, w_gate, w_up, w_down)


def solution(mesh):
    grid_y = mesh.shape['ey']
    grid_x = mesh.shape['ex']
    n_core = mesh.shape['core']
    n = grid_x
    n_dev = grid_y * grid_x * n_core
    chip_list = target_chips(grid_y, grid_x)

    def device_body(tokens, expert_ids, gate_prob, w_gate, w_up, w_down):
        tok_dev, top_k = expert_ids.shape
        exp_dev = w_gate.shape[0]
        exp_chip = exp_dev * n_core
        n_exp = exp_dev * n_dev
        n_copy = tok_dev * top_k
        base_rows = 2 * n_copy // (3 * n_exp)
        hot_rows = grid_y * grid_x * base_rows // 2
        core = lax.axis_index('core')
        iy = lax.axis_index('ey')
        ix = lax.axis_index('ex')
        dst_chip = jnp.where(is_moved(iy, ix, n), lax.rem(iy + n // 2, n) * n + lax.rem(ix + n // 2, n), iy * n + ix)

        key = expert_ids.reshape(n_copy) * n_copy + jnp.arange(n_copy, dtype=jnp.int32)
        skey, sgate = lax.sort((key, gate_prob.reshape(n_copy)), num_keys=1, is_stable=False)
        stok = (lax.rem(skey, n_copy) // top_k).astype(F32)
        tab = jnp.stack([stok, sgate])
        lo = dst_chip * exp_chip
        hot_shift = hot_rows * exp_chip // base_rows
        by_block = tab.reshape(2, n_copy // base_rows, base_rows)
        e_id = jnp.arange(n_exp)[None, :, None]
        base = jnp.where(e_id < lo, by_block[:, :n_exp], by_block[:, hot_shift:hot_shift + n_exp])
        hot = lax.dynamic_slice(tab, (0, lo * base_rows), (2, exp_chip * (base_rows + hot_rows)))
        hot = hot.reshape(2, exp_chip, base_rows + hot_rows)
        base = lax.dynamic_update_slice(base, hot[:, :, :base_rows], (0, lo, 0))
        base = base.reshape(2, n, n, n_core, exp_dev, base_rows)
        base = lax.dynamic_slice_in_dim(jnp.concatenate([base, base], axis=1), iy, n, axis=1)
        base = lax.dynamic_slice_in_dim(jnp.concatenate([base, base], axis=2), ix, n, axis=2)
        base = jnp.where(core == 0, base, base[:, :, :, ::-1])
        hot = hot[:, :, base_rows:].reshape(2, n_core, exp_dev, hot_rows)
        hot = jnp.where(core == 0, hot, hot[:, ::-1])
        n_row = n * n_core * base_rows
        tx = jnp.stack([base.transpose(2, 4, 0, 1, 3, 5).reshape(n, exp_dev * 2, n_row), base.transpose(1, 4, 0, 2, 3, 5).reshape(n, exp_dev * 2, n_row)])
        tx = jnp.pad(tx, ((0, 0), (0, 0), (0, 8 - exp_dev * 2), (0, 0)))
        ht = hot.reshape(2 * exp_chip, hot_rows)

        rx, htr, r1, r2, hk, hr = dispatch(n, n_core, exp_dev, base_rows, hot_rows, tokens, tx, ht)
        r1 = r1.reshape(exp_dev, n, n_core, n, base_rows, -1)
        r2 = r2.reshape(exp_dev, n, n_core, n, base_rows, -1)
        ys = []
        for e in range(exp_dev):
            ys += [y.reshape(n * n_core, n, base_rows, -1) for y in base_ffn(e, r1, r2, w_gate, w_up, w_down)]
        yk, yr = hot_ffn(hk, hr, w_gate, w_up, w_down)
        return combine(n, n_core, tok_dev, rx, htr, ys, yk, yr)

    return jax.shard_map(device_body, mesh=mesh, in_specs=(TOKEN_SPEC, TOKEN_SPEC, TOKEN_SPEC, EXPERT_SPEC, EXPERT_SPEC, EXPERT_SPEC), out_specs=TOKEN_SPEC, check_vma=False)
```

```python
import functools

import jax
import jax.numpy as jnp
from jax import lax
from jax.experimental import pallas as pl
from jax.experimental.pallas import tpu as pltpu
from jax.sharding import PartitionSpec as P

TOKEN_SPEC = P(('dp', 'ey', 'ex', 'core'), None)
EXPERT_SPEC = P(('ey', 'ex', 'core'), None, None)
F32 = jnp.float32
BF16 = jnp.bfloat16
VMEM_LIMIT = 62 * 1024 * 1024
MESH = pl.DeviceIdType.MESH
AXES = (('ex', 'ey'), ('ey', 'ex'))


def target_chips(grid_y, grid_x):
    half_y, half_x = grid_y // 2, grid_x // 2
    chip_list = []
    for chip_y in range(grid_y):
        for chip_x in range(grid_x):
            if chip_y == 0 and chip_x < half_x:
                chip_list.append(half_y * grid_x + chip_x + half_x)
            elif chip_y == half_y and chip_x >= half_x:
                chip_list.append(chip_x - half_x)
            else:
                chip_list.append(chip_y * grid_x + chip_x)
    return chip_list


def is_moved(iy, ix, n):
    half = n // 2
    return ((iy == 0) & (ix < half)) | ((iy == half) & (ix >= half))


def row_to_columns(row):
    return jnp.transpose(jnp.broadcast_to(row, (128, row.shape[1])))


def pick_matrix(row, n_tok):
    cols = row_to_columns(row)
    lane = lax.broadcasted_iota(jnp.int32, cols.shape, 1).astype(F32)
    blocks = [(cols == lane + (128.0 * k)).astype(F32).astype(BF16) for k in range(n_tok // 128)]
    return jnp.concatenate(blocks, axis=1)


def spread_matrix(row, n_tok):
    tok = lax.broadcasted_iota(jnp.int32, (n_tok, row.shape[1]), 0).astype(F32)
    return (tok == row).astype(F32).astype(BF16)


def scaled_rows(rows, gate_row):
    cols = row_to_columns(gate_row)
    reps = rows.shape[1] // 128
    return (rows.astype(F32) * jnp.concatenate([cols] * reps, axis=1)).astype(BF16)


def dot(a, b):
    return jnp.dot(a, b, preferred_element_type=F32)


class Here:
    def __init__(self, n, n_core):
        self.n, self.n_core = n, n_core
        self.iy, self.ix, self.ic = (lax.axis_index(a) for a in ('ey', 'ex', 'core'))
        self.at = {'ey': self.iy, 'ex': self.ix, 'core': self.ic}

    def step(self, axis, by):
        size = self.n_core if axis == 'core' else self.n
        return lax.rem(self.at[axis] + (by % size), size)

    def dev(self, **by):
        return {axis: self.step(axis, k) for axis, k in by.items()}

    def moved(self):
        return is_moved(self.iy, self.ix, self.n)

    def middle(self):
        return is_moved(self.iy, self.step('ex', self.n // 2), self.n)

    def barrier(self):
        sem = pltpu.get_barrier_semaphore()
        peers = [self.dev(**{axis: k, 'core': c}) for axis in ('ey', 'ex') for k in range(1, self.n) for c in range(self.n_core)]
        peers += [self.dev(core=1), self.dev(ey=self.n // 2, ex=self.n // 2)]
        for peer in peers:
            pl.semaphore_signal(sem, inc=1, device_id=peer, device_id_type=MESH)
        pl.semaphore_wait(sem, len(peers))


def remote(src, dst, send_sem, recv_sem, dev):
    return pltpu.make_async_remote_copy(src_ref=src, dst_ref=dst, send_sem=send_sem, recv_sem=recv_sem, device_id=dev, device_id_type=MESH)


def rows_at(start, size):
    return pl.ds(pl.multiple_of(start, size), size)


def load_weights(e, wg_ref, wu_ref, wd_ref, w_ref, sem):
    d_model, d_ff = wg_ref.shape[1:]
    dh = d_model // 2
    copies = [
        pltpu.make_async_copy(wg_ref.at[e], w_ref.at[pl.ds(0, d_model)], sem.at[0]),
        pltpu.make_async_copy(wu_ref.at[e], w_ref.at[pl.ds(d_model, d_model)], sem.at[1]),
        pltpu.make_async_copy(wd_ref.at[e, :, pl.ds(0, dh)], w_ref.at[pl.ds(2 * d_model, d_ff)], sem.at[2]),
        pltpu.make_async_copy(wd_ref.at[e, :, pl.ds(dh, dh)], w_ref.at[pl.ds(2 * d_model + d_ff, d_ff)], sem.at[3]),
    ]
    for c in copies:
        c.start()
    return copies


def gated_mlp(x1, x2, w_ref, d_model, d_ff):
    dh = d_model // 2
    gate = dot(x1, w_ref[0:dh]) + dot(x2, w_ref[dh:d_model])
    up = dot(x1, w_ref[d_model:d_model + dh]) + dot(x2, w_ref[d_model + dh:2 * d_model])
    hidden = (jax.nn.silu(gate) * up).astype(BF16)
    y1 = dot(hidden, w_ref[2 * d_model:2 * d_model + d_ff]).astype(BF16)
    y2 = dot(hidden, w_ref[2 * d_model + d_ff:2 * d_model + 2 * d_ff]).astype(BF16)
    return y1, y2


def return_copy(here, h, j, src, dst, s_sem, r_sem, piece):
    rows = rows_at(j * piece, piece)
    axis = AXES[h][1]
    size = here.n_core
    dev = here.dev(**{axis: here.n - j // size, 'core': j % size})
    return remote(src.at[h, rows], dst.at[h, rows], s_sem.at[h, j], r_sem.at[h, j], dev)


def return_keep(h, src, dst, s_sem, piece):
    rows = pl.ds(0, piece)
    return pltpu.make_async_copy(src.at[h, rows], dst.at[h, rows], s_sem.at[h, 0])


def base_ffn(here, x_ref, dst_ref, w_ref, d_model, d_ff, base_rows, s_sem, r_sem):
    n, n_core = here.n, here.n_core
    piece = n * base_rows

    @pl.loop(0, n * n_core)
    def _(t):
        dc, dy = t // n, lax.rem(t, n)
        j = dy * n_core + dc
        rows1 = rows_at(j * piece, piece)
        rows2 = [rows_at((dx * n_core + dc) * piece + dy * base_rows, base_rows) for dx in range(n)]
        x2 = jnp.concatenate([x_ref[1, r] for r in rows2], axis=0)
        y1, y2 = gated_mlp(x_ref[0, rows1], x2, w_ref, d_model, d_ff)
        x_ref[0, rows1] = y1
        for dx in range(n):
            x_ref[1, rows2[dx]] = y2[dx * base_rows:(dx + 1) * base_rows]

        @pl.when(j > 0)
        def _():
            return_copy(here, 0, j, x_ref, dst_ref, s_sem, r_sem, piece).start()

        @pl.when(j == 0)
        def _():
            return_keep(0, x_ref, dst_ref, s_sem, piece).start()

        @pl.when(dy == n - 1)
        def _():
            for dx in range(n - 1, 0, -1):
                return_copy(here, 1, dx * n_core + dc, x_ref, dst_ref, s_sem, r_sem, piece).start()

            @pl.when(dc > 0)
            def _():
                return_copy(here, 1, dc, x_ref, dst_ref, s_sem, r_sem, piece).start()

            @pl.when(dc == 0)
            def _():
                return_keep(1, x_ref, dst_ref, s_sem, piece).start()


def wait_return_sends(here, x_ref, dst_ref, base_rows, s_sem, r_sem):
    piece = here.n * base_rows
    for h in range(2):
        return_keep(h, x_ref, dst_ref, s_sem, piece).wait()
        for j in range(1, here.n * here.n_core):
            return_copy(here, h, j, x_ref, dst_ref, s_sem, r_sem, piece).wait_send()


def wait_return_recvs(here, x_ref, dst_ref, base_rows, s_sem, r_sem):
    piece = here.n * base_rows
    for h in range(2):
        for j in range(1, here.n * here.n_core):
            return_copy(here, h, j, x_ref, dst_ref, s_sem, r_sem, piece).wait_recv()


def dispatch_kernel(n, n_core, exp_dev, base_rows, hot_rows, tok_ref, tx_ref, ht_ref, wg_ref, wu_ref, wd_ref,
                    rx_ref, htr_ref, re_ref, q_ref, hyk_ref, hyb_ref,
                    g_ref, hb_ref, sb_ref, rv_ref, hr_ref, w_ref,
                    own_sem, w_sem, tab_s, tab_r, g_s, g_r, d_s, d_r, hot_s, hot_r, swap_s, swap_r, keep_sem, ret_s, ret_r):
    here = Here(n, n_core)
    tok_dev, d_model = tok_ref.shape
    d_ff = wg_ref.shape[2]
    dh = d_model // 2
    half = tok_dev // 2
    lo, hi = pl.ds(0, half), pl.ds(half, half)
    n_dst = n * n_core
    piece = n * base_rows
    own = [pltpu.make_async_copy(tok_ref.at[:, pl.ds(h * dh, dh)], g_ref.at[h, 0], own_sem.at[h]) for h in range(2)]
    for c in own:
        c.start()
    here.barrier()

    tabs = []
    for h in range(2):
        rx_ref[h, 0] = tx_ref[h, 0]
        for k in range(1, n):
            c = remote(tx_ref.at[h, k], rx_ref.at[h, k], tab_s.at[h * n + k], tab_r.at[h * n + k], here.dev(**{AXES[h][0]: k}))
            c.start()
            tabs.append(c)
    moved = here.moved()
    middle = here.middle()
    hot_tab = remote(ht_ref, htr_ref, tab_s.at[0], tab_r.at[0], here.dev(ey=n // 2, ex=n // 2))

    @pl.when(moved)
    def _():
        hot_tab.start()

    @pl.when(jnp.logical_not(moved))
    def _():
        htr_ref[...] = ht_ref[...]

    first = []
    for h in range(2):
        own[h].wait()
        axis = AXES[h][0]
        for i, (slot, rows, by) in enumerate(((1, lo, 1), (3, hi, -1), (1, hi, 1), (3, lo, -1))):
            c = remote(g_ref.at[h, 0, rows], g_ref.at[h, slot, rows], g_s.at[h, i], g_r.at[h, i], here.dev(**{axis: by}))
            c.start()
            first.append(c)
    weights = load_weights(0, wg_ref, wu_ref, wd_ref, w_ref, w_sem)
    for c in tabs:
        c.wait_recv()

    def pick(s, start, stop):
        @pl.loop(start, stop)
        def _(m):
            e, h = m // 2, lax.rem(m, 2)
            mat = pick_matrix(rx_ref[h, s, pl.ds(2 * e, 1)], tok_dev)
            picked = dot(mat, g_ref[h, s]).astype(BF16)
            for j in range(n_dst):
                sb_ref[h, e, pl.ds(j * piece + s * base_rows, base_rows)] = picked[j * base_rows:(j + 1) * base_rows]

    pick(0, 0, 2 * exp_dev)
    far = []
    for i, (slot, rows, by) in enumerate(((1, lo, 1), (3, hi, -1))):
        for h in range(2):
            first[h * 4 + i].wait_recv()
            c = remote(g_ref.at[h, slot, rows], g_ref.at[h, 2, rows], g_s.at[h, 4 + i], g_r.at[h, 4 + i], here.dev(**{AXES[h][0]: by}))
            c.start()
            far.append(c)
    for i, slot in enumerate((1, 3)):
        for h in range(2):
            first[h * 4 + 2 + i].wait_recv()
        pick(slot, 0, 2 * exp_dev)
    for c in far:
        c.wait_recv()

    hot = [remote(g_ref.at[h, 2], hb_ref.at[h], hot_s.at[h], hot_r.at[h], here.dev(**{AXES[h][1]: n // 2})) for h in range(2)]
    sends = []
    for e in range(exp_dev):
        pick(2, 2 * e, 2 * e + 2)
        dst = rv_ref if e == 0 else re_ref
        for j in range(n_dst - 1, -1, -1):
            for h in range(2):
                rows = pl.ds(j * piece, piece)
                if j:
                    c = remote(sb_ref.at[h, e, rows], dst.at[h, rows], d_s.at[h, e, j], d_r.at[h, e, j], here.dev(**{AXES[h][1]: j // n_core, 'core': j % n_core}))
                else:
                    c = pltpu.make_async_copy(sb_ref.at[h, e, rows], dst.at[h, rows], d_s.at[h, e, j])
                c.start()
                sends.append(c)
        if e == 0:
            @pl.when(middle)
            def _():
                for c in hot:
                    c.start()

    n_first = 2 * n_dst
    for c in weights:
        c.wait()
    for c in sends[:n_first]:
        if c.is_remote:
            c.wait_recv()
        else:
            c.wait()
    base_ffn(here, rv_ref, q_ref, w_ref, d_model, d_ff, base_rows, ret_s, ret_r)

    @pl.when(jnp.logical_not(moved))
    def _():
        for h in range(2):
            hb_ref[h] = g_ref[h, 0]

    @pl.when(moved)
    def _():
        hot_tab.wait_recv()
        for c in hot:
            c.wait_recv()

    for c in sends[:n_first]:
        if c.is_remote:
            c.wait_send()
    hot_dev = exp_dev * hot_rows
    swap = []
    for rel in range(n_core - 1, -1, -1):
        @pl.loop(0, exp_dev)
        def _(e):
            mat = pick_matrix(htr_ref[pl.ds(rel * exp_dev + e, 1)], tok_dev)
            for h in range(2):
                sb_ref[h, 0, rows_at(rel * hot_dev + e * hot_rows, hot_rows)] = dot(mat, hb_ref[h]).astype(BF16)

        if rel:
            for h in range(2):
                c = remote(sb_ref.at[h, 0, pl.ds(hot_dev, hot_dev)], hr_ref.at[h], swap_s.at[h], swap_r.at[h], here.dev(core=rel))
                c.start()
                swap.append(c)

    tile = piece

    def hot_tiles(e, ref, pre):
        @pl.loop(0, hot_rows // tile)
        def _(k):
            rows = rows_at(e * hot_rows + k * tile, tile)
            y1, y2 = gated_mlp(ref[pre(0) + (rows,)], ref[pre(1) + (rows,)], w_ref, d_model, d_ff)
            ref[pre(0) + (rows,)] = y1
            ref[pre(1) + (rows,)] = y2

    @pl.loop(0, exp_dev)
    def _(e):
        @pl.when(e > 0)
        def _():
            for c in load_weights(e, wg_ref, wu_ref, wd_ref, w_ref, w_sem):
                c.wait()

        hot_tiles(e, sb_ref, lambda h: (h, 0))

        @pl.when(e == 0)
        def _():
            for c in swap:
                c.wait_recv()

        hot_tiles(e, hr_ref, lambda h: (h,))

    back = []
    for h in range(2):
        c = remote(hr_ref.at[h], hyb_ref.at[h], swap_s.at[2 + h], swap_r.at[2 + h], here.dev(core=1))
        c.start()
        back.append(c)
        c = pltpu.make_async_copy(sb_ref.at[h, 0, pl.ds(0, hot_dev)], hyk_ref.at[h], keep_sem.at[h])
        c.start()
        back.append(c)

    for c in sends[n_first:]:
        if c.is_remote:
            c.wait_send()
            c.wait_recv()
        else:
            c.wait()
    for c in tabs + first + far + swap:
        c.wait_send()
    wait_return_sends(here, rv_ref, q_ref, base_rows, ret_s, ret_r)
    wait_return_recvs(here, rv_ref, q_ref, base_rows, ret_s, ret_r)
    for c in back:
        if c.is_remote:
            c.wait_send()
            c.wait_recv()
        else:
            c.wait()

    @pl.when(moved)
    def _():
        hot_tab.wait_send()

    @pl.when(middle)
    def _():
        for c in hot:
            c.wait_send()


def dispatch(n, n_core, base_rows, hot_rows, tokens, tx, ht, w_gate, w_up, w_down):
    tok_dev, d_model = tokens.shape
    exp_dev, _, d_ff = w_gate.shape
    dh = d_model // 2
    n_dst = n * n_core
    n_row = n_dst * n * base_rows
    any_ = pl.BlockSpec(memory_space=pl.ANY)
    vm = pl.BlockSpec(memory_space=pltpu.VMEM)
    rows = jax.ShapeDtypeStruct((2, n_row, dh), BF16)
    hot = jax.ShapeDtypeStruct((2, exp_dev * hot_rows, dh), BF16)
    dma = pltpu.SemaphoreType.DMA
    return pl.pallas_call(
        functools.partial(dispatch_kernel, n, n_core, exp_dev, base_rows, hot_rows),
        out_shape=(jax.ShapeDtypeStruct(tx.shape, F32), jax.ShapeDtypeStruct(ht.shape, F32), rows, rows, hot, hot),
        in_specs=[any_, vm, vm, any_, any_, any_],
        out_specs=(vm, vm, any_, any_, any_, any_),
        scratch_shapes=[
            pltpu.VMEM((2, n, tok_dev, dh), BF16),
            pltpu.VMEM((2, tok_dev, dh), BF16),
            pltpu.VMEM((2, exp_dev, n_row, dh), BF16),
            pltpu.VMEM((2, n_row, dh), BF16),
            pltpu.VMEM((2, exp_dev * hot_rows, dh), BF16),
            pltpu.VMEM((2 * d_model + 2 * d_ff, dh), BF16),
            dma((2,)), dma((4,)), dma((2 * n,)), dma((2 * n,)), dma((2, 6)), dma((2, 6)),
            dma((2, exp_dev, n_dst)), dma((2, exp_dev, n_dst)), dma((2,)), dma((2,)), dma((4,)), dma((4,)), dma((2,)),
            dma((2, n_dst)), dma((2, n_dst)),
        ],
        compiler_params=pltpu.CompilerParams(vmem_limit_bytes=VMEM_LIMIT, collective_id=0, has_side_effects=True),
        name='dispatch',
    )(tokens, tx, ht, w_gate, w_up, w_down)


def combine_kernel(n, n_core, exp_dev, base_rows, hot_rows, rx_ref, htr_ref, re_ref, qe_ref, hyk_ref, hyb_ref, wg_ref, wu_ref, wd_ref, out_ref,
                   x_ref, q_ref, w_ref, s_ref, hs_ref, u_ref, v_ref,
                   x_sem, q_sem, w_sem, hy_sem, out_sem, hot_s, hot_r, ring_s, ring_r, ret_s, ret_r):
    here = Here(n, n_core)
    tok_dev, d_model = out_ref.shape
    d_ff = wg_ref.shape[2]
    dh = d_model // 2
    half = tok_dev // 2
    lo, hi = pl.ds(0, half), pl.ds(half, half)
    n_dst = n * n_core
    piece = n * base_rows
    weights = load_weights(exp_dev - 1, wg_ref, wu_ref, wd_ref, w_ref, w_sem)
    x_in = pltpu.make_async_copy(re_ref, x_ref, x_sem)
    x_in.start()
    q_in = pltpu.make_async_copy(qe_ref, q_ref.at[0], q_sem)
    hot_dev = exp_dev * hot_rows
    hot_in = [pltpu.make_async_copy(src.at[h], q_ref.at[0, h, pl.ds(i * hot_dev, hot_dev)], hy_sem.at[h, i]) for h in range(2) for i, src in enumerate((hyk_ref, hyb_ref))]
    for c in hot_in:
        c.start()
    here.barrier()
    moved = here.moved()
    middle = here.middle()
    x_in.wait()
    for c in weights:
        c.wait()
    base_ffn(here, x_ref, q_ref.at[1], w_ref, d_model, d_ff, base_rows, ret_s, ret_r)

    acc = None
    hot = [remote(s_ref.at[h], hs_ref.at[h], hot_s.at[h], hot_r.at[h], here.dev(**{AXES[h][1]: n // 2})) for h in range(2)]
    for c in hot_in:
        c.wait()
    for h, k in [(h, k) for h in range(2) for k in range(n_core * exp_dev)]:
        rows = scaled_rows(q_ref[0, h, pl.ds(k * hot_rows, hot_rows)], htr_ref[n_core * exp_dev + k:n_core * exp_dev + k + 1])
        term = dot(spread_matrix(htr_ref[k:k + 1], tok_dev), rows)
        acc = term if k == 0 else acc + term
        if k == n_core * exp_dev - 1:
            s_ref[h] = acc.astype(BF16)

            @pl.when(moved)
            def _():
                hot[h].start()

    q_in.start()
    q_in.wait()
    for h in range(2):
        return_keep(h, x_ref, q_ref.at[1], ret_s, piece).wait()
    wait_return_recvs(here, x_ref, q_ref.at[1], base_rows, ret_s, ret_r)

    def p_rows(h, s, part=None):
        start = (h * n + s) * tok_dev
        return pl.ds(start, tok_dev) if part is None else pl.ds(start + part * half, half)

    def spread(h, s):
        acc = None
        for e in range(exp_dev):
            rows = jnp.concatenate([q_ref[e, h, pl.ds(j * piece + s * base_rows, base_rows)] for j in range(n_dst)], axis=0)
            term = dot(spread_matrix(rx_ref[h, s, pl.ds(2 * e, 1)], tok_dev), scaled_rows(rows, rx_ref[h, s, pl.ds(2 * e + 1, 1)]))
            acc = term if acc is None else acc + term
        return acc

    ring = []

    def send(h, i, src, dst, by, start=True):
        c = remote(src, dst, ring_s.at[h, i], ring_r.at[h, i], here.dev(**{AXES[h][0]: by}))
        if start:
            c.start()
        ring.append(c)
        return c

    far = []
    for h in range(2):
        w_ref[p_rows(h, 2)] = spread(h, 2).astype(BF16)
        far.append(send(h, 0, w_ref.at[p_rows(h, 2, 0)], u_ref.at[h, lo], 1, False))
        far.append(send(h, 1, w_ref.at[p_rows(h, 2, 1)], u_ref.at[h, hi], -1, False))

        @pl.when(jnp.logical_not(middle))
        def _():
            far[2 * h].start()
            far[2 * h + 1].start()

    last = []
    for h in range(2):
        w_ref[p_rows(h, 3)] = spread(h, 3).astype(BF16)
        last.append(send(h, 2, w_ref.at[p_rows(h, 3, 1)], v_ref.at[h, 0, hi], 1))
        w_ref[p_rows(h, 1)] = spread(h, 1).astype(BF16)
        last.append(send(h, 3, w_ref.at[p_rows(h, 1, 0)], v_ref.at[h, 1, lo], -1))

    @pl.when(middle)
    def _():
        for h in range(2):
            hot[h].wait_recv()
            w_ref[p_rows(h, 2)] = (w_ref[p_rows(h, 2)].astype(F32) + hs_ref[h].astype(F32)).astype(BF16)
            far[2 * h].start()
            far[2 * h + 1].start()

    own_hot = jnp.where(moved, 0.0, 1.0).astype(F32)
    for h in range(2):
        w_ref[p_rows(h, 0)] = (spread(h, 0) + own_hot * s_ref[h].astype(F32)).astype(BF16)
    for h in range(2):
        far[2 * h].wait_recv()
        w_ref[p_rows(h, 3, 0)] = (w_ref[p_rows(h, 3, 0)].astype(F32) + u_ref[h, lo].astype(F32)).astype(BF16)
        last.append(send(h, 4, w_ref.at[p_rows(h, 3, 0)], v_ref.at[h, 0, lo], 1))
        far[2 * h + 1].wait_recv()
        w_ref[p_rows(h, 1, 1)] = (w_ref[p_rows(h, 1, 1)].astype(F32) + u_ref[h, hi].astype(F32)).astype(BF16)
        last.append(send(h, 5, w_ref.at[p_rows(h, 1, 1)], v_ref.at[h, 1, hi], -1))
    for c in last:
        c.wait_recv()
    for h in range(2):
        w_ref[p_rows(h, 0)] = (w_ref[p_rows(h, 0)].astype(F32) + v_ref[h, 0].astype(F32) + v_ref[h, 1].astype(F32)).astype(BF16)
        done = pltpu.make_async_copy(w_ref.at[p_rows(h, 0)], out_ref.at[:, pl.ds(h * dh, dh)], out_sem.at[h])
        done.start()
        last.append(done)

    for h in range(2):
        last[-1 - h].wait()
        for j in range(1, n_dst):
            return_copy(here, h, j, x_ref, q_ref.at[1], ret_s, ret_r, piece).wait_send()
    for c in ring:
        c.wait_send()

    @pl.when(moved)
    def _():
        for c in hot:
            c.wait_send()


def combine(n, n_core, tok_dev, base_rows, hot_rows, rx, htr, re, qe, hyk, hyb, w_gate, w_up, w_down):
    exp_dev, d_model, d_ff = w_gate.shape
    _, n_row, dh = re.shape
    n_dst = n * n_core
    any_ = pl.BlockSpec(memory_space=pl.ANY)
    vm = pl.BlockSpec(memory_space=pltpu.VMEM)
    dma = pltpu.SemaphoreType.DMA
    tok_buf = pltpu.VMEM((2, tok_dev, dh), BF16)
    w_rows = max(2 * d_model + 2 * d_ff, 2 * n * tok_dev)
    return pl.pallas_call(
        functools.partial(combine_kernel, n, n_core, exp_dev, base_rows, hot_rows),
        out_shape=jax.ShapeDtypeStruct((tok_dev, d_model), BF16),
        in_specs=[vm, vm] + [any_] * 7,
        out_specs=any_,
        scratch_shapes=[
            pltpu.VMEM((2, n_row, dh), BF16),
            pltpu.VMEM((exp_dev, 2, n_row, dh), BF16),
            pltpu.VMEM((w_rows, dh), BF16),
            tok_buf, tok_buf, tok_buf,
            pltpu.VMEM((2, 2, tok_dev, dh), BF16),
            dma, dma, dma((4,)), dma((2, 2)), dma((2,)), dma((2,)), dma((2,)), dma((2, 6)), dma((2, 6)), dma((2, n_dst)), dma((2, n_dst)),
        ],
        compiler_params=pltpu.CompilerParams(vmem_limit_bytes=VMEM_LIMIT, collective_id=1, has_side_effects=True),
        name='combine',
    )(rx, htr, re, qe, hyk, hyb, w_gate, w_up, w_down)


def solution(mesh):
    grid_y = mesh.shape['ey']
    grid_x = mesh.shape['ex']
    n_core = mesh.shape['core']
    n = grid_x
    n_dev = grid_y * grid_x * n_core
    chip_list = target_chips(grid_y, grid_x)

    def device_body(tokens, expert_ids, gate_prob, w_gate, w_up, w_down):
        tok_dev, top_k = expert_ids.shape
        exp_dev = w_gate.shape[0]
        exp_chip = exp_dev * n_core
        n_exp = exp_dev * n_dev
        n_copy = tok_dev * top_k
        base_rows = 2 * n_copy // (3 * n_exp)
        hot_rows = grid_y * grid_x * base_rows // 2
        core = lax.axis_index('core')
        iy = lax.axis_index('ey')
        ix = lax.axis_index('ex')
        dst_chip = jnp.where(is_moved(iy, ix, n), lax.rem(iy + n // 2, n) * n + lax.rem(ix + n // 2, n), iy * n + ix)

        key = expert_ids.reshape(n_copy) * n_copy + jnp.arange(n_copy, dtype=jnp.int32)
        skey, sgate = lax.sort((key, gate_prob.reshape(n_copy)), num_keys=1, is_stable=False)
        stok = (lax.rem(skey, n_copy) // top_k).astype(F32)
        tab = jnp.stack([stok, sgate])
        lo = dst_chip * exp_chip
        hot_shift = hot_rows * exp_chip // base_rows
        by_block = tab.reshape(2, n_copy // base_rows, base_rows)
        e_id = jnp.arange(n_exp)[None, :, None]
        base = jnp.where(e_id < lo, by_block[:, :n_exp], by_block[:, hot_shift:hot_shift + n_exp])
        hot = lax.dynamic_slice(tab, (0, lo * base_rows), (2, exp_chip * (base_rows + hot_rows)))
        hot = hot.reshape(2, exp_chip, base_rows + hot_rows)
        base = lax.dynamic_update_slice(base, hot[:, :, :base_rows], (0, lo, 0))
        base = base.reshape(2, n, n, n_core, exp_dev, base_rows)
        base = lax.dynamic_slice_in_dim(jnp.concatenate([base, base], axis=1), iy, n, axis=1)
        base = lax.dynamic_slice_in_dim(jnp.concatenate([base, base], axis=2), ix, n, axis=2)
        base = jnp.where(core == 0, base, base[:, :, :, ::-1])
        hot = hot[:, :, base_rows:].reshape(2, n_core, exp_dev, hot_rows)
        hot = jnp.where(core == 0, hot, hot[:, ::-1])
        n_row = n * n_core * base_rows
        tx = jnp.stack([base.transpose(2, 4, 0, 1, 3, 5).reshape(n, exp_dev * 2, n_row), base.transpose(1, 4, 0, 2, 3, 5).reshape(n, exp_dev * 2, n_row)])
        tx = jnp.pad(tx, ((0, 0), (0, 0), (0, 8 - exp_dev * 2), (0, 0)))
        ht = hot.reshape(2 * exp_chip, hot_rows)

        rx, htr, re, qe, hyk, hyb = dispatch(n, n_core, base_rows, hot_rows, tokens, tx, ht, w_gate, w_up, w_down)
        return combine(n, n_core, tok_dev, base_rows, hot_rows, rx, htr, re, qe, hyk, hyb, w_gate, w_up, w_down)

    return jax.shard_map(device_body, mesh=mesh, in_specs=(TOKEN_SPEC, TOKEN_SPEC, TOKEN_SPEC, EXPERT_SPEC, EXPERT_SPEC, EXPERT_SPEC), out_specs=TOKEN_SPEC, check_vma=False)
```

```python
import functools

import jax
import jax.numpy as jnp
from jax import lax
from jax.experimental import pallas as pl
from jax.experimental.pallas import tpu as pltpu
from jax.sharding import PartitionSpec as P

TOKEN_SPEC = P(('dp', 'ey', 'ex', 'core'), None)
EXPERT_SPEC = P(('ey', 'ex', 'core'), None, None)
F32 = jnp.float32
BF16 = jnp.bfloat16
VMEM_LIMIT = 62 * 1024 * 1024
MESH = pl.DeviceIdType.MESH
AXES = (('ex', 'ey'), ('ey', 'ex'))


def target_chips(grid_y, grid_x):
    half_y, half_x = grid_y // 2, grid_x // 2
    chip_list = []
    for chip_y in range(grid_y):
        for chip_x in range(grid_x):
            if chip_y == 0 and chip_x < half_x:
                chip_list.append(half_y * grid_x + chip_x + half_x)
            elif chip_y == half_y and chip_x >= half_x:
                chip_list.append(chip_x - half_x)
            else:
                chip_list.append(chip_y * grid_x + chip_x)
    return chip_list


def is_moved(iy, ix, n):
    half = n // 2
    return ((iy == 0) & (ix < half)) | ((iy == half) & (ix >= half))


def row_to_columns(row):
    return jnp.transpose(jnp.broadcast_to(row, (128, row.shape[1])))


def pick_matrix(row, n_tok):
    cols = row_to_columns(row)
    lane = lax.broadcasted_iota(jnp.int32, cols.shape, 1).astype(F32)
    blocks = [(cols == lane + (128.0 * k)).astype(F32).astype(BF16) for k in range(n_tok // 128)]
    return jnp.concatenate(blocks, axis=1)


def spread_matrix(row, n_tok):
    tok = lax.broadcasted_iota(jnp.int32, (n_tok, row.shape[1]), 0).astype(F32)
    return (tok == row).astype(F32).astype(BF16)


def scaled_rows(rows, gate_row):
    cols = row_to_columns(gate_row)
    reps = rows.shape[1] // 128
    return (rows.astype(F32) * jnp.concatenate([cols] * reps, axis=1)).astype(BF16)


def dot(a, b):
    return jnp.dot(a, b, preferred_element_type=F32)


class Here:
    def __init__(self, n, n_core):
        self.n, self.n_core = n, n_core
        self.iy, self.ix, self.ic = (lax.axis_index(a) for a in ('ey', 'ex', 'core'))
        self.at = {'ey': self.iy, 'ex': self.ix, 'core': self.ic}

    def step(self, axis, by):
        size = self.n_core if axis == 'core' else self.n
        return lax.rem(self.at[axis] + (by % size), size)

    def dev(self, **by):
        return {axis: self.step(axis, k) for axis, k in by.items()}

    def moved(self):
        return is_moved(self.iy, self.ix, self.n)

    def middle(self):
        return is_moved(self.iy, self.step('ex', self.n // 2), self.n)

    def barrier(self):
        sem = pltpu.get_barrier_semaphore()
        peers = [self.dev(**{axis: k, 'core': c}) for axis in ('ey', 'ex') for k in range(1, self.n) for c in range(self.n_core)]
        peers += [self.dev(core=1), self.dev(ey=self.n // 2, ex=self.n // 2)]
        for peer in peers:
            pl.semaphore_signal(sem, inc=1, device_id=peer, device_id_type=MESH)
        pl.semaphore_wait(sem, len(peers))


def remote(src, dst, send_sem, recv_sem, dev):
    return pltpu.make_async_remote_copy(src_ref=src, dst_ref=dst, send_sem=send_sem, recv_sem=recv_sem, device_id=dev, device_id_type=MESH)


def rows_at(start, size):
    return pl.ds(pl.multiple_of(start, size), size)


def load_weights(e, wg_ref, wu_ref, wd_ref, w_ref, sem):
    d_model, d_ff = wg_ref.shape[1:]
    dh = d_model // 2
    copies = [
        pltpu.make_async_copy(wg_ref.at[e], w_ref.at[pl.ds(0, d_model)], sem.at[0]),
        pltpu.make_async_copy(wu_ref.at[e], w_ref.at[pl.ds(d_model, d_model)], sem.at[1]),
        pltpu.make_async_copy(wd_ref.at[e, :, pl.ds(0, dh)], w_ref.at[pl.ds(2 * d_model, d_ff)], sem.at[2]),
        pltpu.make_async_copy(wd_ref.at[e, :, pl.ds(dh, dh)], w_ref.at[pl.ds(2 * d_model + d_ff, d_ff)], sem.at[3]),
    ]
    for c in copies:
        c.start()
    return copies


def gated_mlp(x1, x2, w_ref, d_model, d_ff):
    dh = d_model // 2
    gate = dot(x1, w_ref[0:dh]) + dot(x2, w_ref[dh:d_model])
    up = dot(x1, w_ref[d_model:d_model + dh]) + dot(x2, w_ref[d_model + dh:2 * d_model])
    hidden = (jax.nn.silu(gate) * up).astype(BF16)
    y1 = dot(hidden, w_ref[2 * d_model:2 * d_model + d_ff]).astype(BF16)
    y2 = dot(hidden, w_ref[2 * d_model + d_ff:2 * d_model + 2 * d_ff]).astype(BF16)
    return y1, y2


def place(off, n):
    if isinstance(off, int):
        return off if off < n // 2 else (n - 1 if off == n // 2 else off - 1)
    return jnp.where(off < n // 2, off, jnp.where(off == n // 2, n - 1, off - 1))


def return_copy(here, h, j, src, start, dst, s_sem, r_sem, piece):
    axis = AXES[h][1]
    size = here.n_core
    dev = here.dev(**{axis: here.n - j // size, 'core': j % size})
    return remote(src.at[h, rows_at(start + j * piece, piece)], dst.at[h, rows_at(j * piece, piece)], s_sem.at[h, j], r_sem.at[h, j], dev)


def return_keep(h, src, start, dst, s_sem, piece):
    return pltpu.make_async_copy(src.at[h, pl.ds(start, piece)], dst.at[h, pl.ds(0, piece)], s_sem.at[h, 0])


def base_ffn(here, x_ref, start, dst_ref, w_ref, d_model, d_ff, base_rows, s_sem, r_sem):
    n, n_core = here.n, here.n_core
    piece = n * base_rows

    @pl.loop(0, n * n_core)
    def _(t):
        dc, dy = t // n, lax.rem(t, n)
        j = dy * n_core + dc
        rows1 = rows_at(start + j * piece, piece)
        rows2 = [None] * n
        for dx in range(n):
            rows2[place(dx, n)] = rows_at(start + (dx * n_core + dc) * piece + place(dy, n) * base_rows, base_rows)
        x2 = jnp.concatenate([x_ref[1, r] for r in rows2], axis=0)
        y1, y2 = gated_mlp(x_ref[0, rows1], x2, w_ref, d_model, d_ff)
        x_ref[0, rows1] = y1
        for i in range(n):
            x_ref[1, rows2[i]] = y2[i * base_rows:(i + 1) * base_rows]

        @pl.when(j > 0)
        def _():
            return_copy(here, 0, j, x_ref, start, dst_ref, s_sem, r_sem, piece).start()

        @pl.when(j == 0)
        def _():
            return_keep(0, x_ref, start, dst_ref, s_sem, piece).start()

        @pl.when(dy == n - 1)
        def _():
            for dx in range(n - 1, 0, -1):
                return_copy(here, 1, dx * n_core + dc, x_ref, start, dst_ref, s_sem, r_sem, piece).start()

            @pl.when(dc > 0)
            def _():
                return_copy(here, 1, dc, x_ref, start, dst_ref, s_sem, r_sem, piece).start()

            @pl.when(dc == 0)
            def _():
                return_keep(1, x_ref, start, dst_ref, s_sem, piece).start()


def layer_kernel(n, n_core, exp_dev, base_rows, hot_rows, tok_ref, tx_ref, ht_ref, wg_ref, wu_ref, wd_ref,
                 p0_ref, v_ref, re_ref, q_ref, hs_ref, u_ref, hy_ref,
                 rx_ref, htr_ref, g_ref, hb_ref, m_ref, w_ref,
                 own_sem, w_sem, tab_s, tab_r, g_s, g_r, d_s, d_r, hot_s, hot_r, swap_s, swap_r, x_sem, ret_s, ret_r, sum_s, sum_r, ring_s, ring_r, load_sem):
    here = Here(n, n_core)
    tok_dev, d_model = tok_ref.shape
    d_ff = wg_ref.shape[2]
    dh = d_model // 2
    half = tok_dev // 2
    n_dst = n * n_core
    piece = n * base_rows
    n_row = n_dst * piece
    hot_dev = exp_dev * hot_rows
    land = exp_dev * n_row
    recv0 = land + hot_dev
    far_slot = n // 2
    lo, hi = pl.ds(0, half), pl.ds(half, half)

    def slot(s, part=None):
        return pl.ds(s * tok_dev, tok_dev) if part is None else pl.ds(s * tok_dev + part * half, half)

    own = [pltpu.make_async_copy(tok_ref.at[:, pl.ds(h * dh, dh)], g_ref.at[h, slot(0)], own_sem.at[h]) for h in range(2)]
    for c in own:
        c.start()
    here.barrier()

    tabs = []
    for h in range(2):
        rx_ref[h, 0] = tx_ref[h, 0]
        for k in range(1, n):
            c = remote(tx_ref.at[h, k], rx_ref.at[h, k], tab_s.at[h * n + k], tab_r.at[h * n + k], here.dev(**{AXES[h][0]: k}))
            c.start()
            tabs.append(c)
    moved = here.moved()
    middle = here.middle()
    hot_tab = remote(ht_ref, htr_ref, tab_s.at[0], tab_r.at[0], here.dev(ey=n // 2, ex=n // 2))

    @pl.when(moved)
    def _():
        hot_tab.start()

    @pl.when(jnp.logical_not(moved))
    def _():
        htr_ref[...] = ht_ref[...]

    first = []
    for h in range(2):
        own[h].wait()
        axis = AXES[h][0]
        for i, (s, part, by) in enumerate(((1, 0, 1), (n - 1, 1, -1), (1, 1, 1), (n - 1, 0, -1))):
            c = remote(g_ref.at[h, slot(0, part)], g_ref.at[h, slot(s, part)], g_s.at[h, i], g_r.at[h, i], here.dev(**{axis: by}))
            c.start()
            first.append(c)
    weights = load_weights(0, wg_ref, wu_ref, wd_ref, w_ref, w_sem)
    for c in tabs:
        c.wait_recv()

    def pick(s, start, stop):
        @pl.loop(start, stop)
        def _(m):
            e, h = m // 2, lax.rem(m, 2)
            mat = pick_matrix(rx_ref[h, s, pl.ds(2 * e, 1)], tok_dev)
            picked = dot(mat, g_ref[h, slot(s)]).astype(BF16)
            for j in range(n_dst):
                m_ref[h, rows_at(e * n_row + j * piece + place(s, n) * base_rows, base_rows)] = picked[j * base_rows:(j + 1) * base_rows]

    sends = [[], []]

    def send_rows(e, first_row, size, i, keep):
        for j in range(n_dst - 1, -1 if keep else 0, -1):
            for h in range(2):
                if j:
                    src = m_ref.at[h, pl.ds(e * n_row + j * piece + first_row, size)]
                    dst = m_ref.at[h, pl.ds(recv0 + j * piece + first_row, size)] if e == 0 else re_ref.at[h, pl.ds(j * piece + first_row, size)]
                    c = remote(src, dst, d_s.at[h, e, j, i], d_r.at[h, e, j, i], here.dev(**{AXES[h][1]: j // n_core, 'core': j % n_core}))
                else:
                    dst = m_ref.at[h, pl.ds(recv0, piece)] if e == 0 else re_ref.at[h, pl.ds(0, piece)]
                    c = pltpu.make_async_copy(m_ref.at[h, pl.ds(e * n_row, piece)], dst, d_s.at[h, e, j, i])
                c.start()
                sends[e].append(c)

    pick(0, 0, 2 * exp_dev)
    far = []
    for i, (s, part, by) in enumerate(((1, 0, 1), (n - 1, 1, -1))):
        for h in range(2):
            first[h * 4 + i].wait_recv()
            c = remote(g_ref.at[h, slot(s, part)], g_ref.at[h, slot(far_slot, part)], g_s.at[h, 4 + i], g_r.at[h, 4 + i], here.dev(**{AXES[h][0]: by}))
            c.start()
            far.append(c)
    for i, s in enumerate((1, n - 1)):
        for h in range(2):
            first[h * 4 + 2 + i].wait_recv()
        pick(s, 0, 2 * exp_dev)
    send_rows(0, 0, piece - base_rows, 0, False)
    for c in far:
        c.wait_recv()
    pick(far_slot, 0, 2)
    send_rows(0, piece - base_rows, base_rows, 1, True)

    hot = [remote(g_ref.at[h, slot(far_slot)], hb_ref.at[h], hot_s.at[h], hot_r.at[h], here.dev(**{AXES[h][1]: n // 2})) for h in range(2)]

    @pl.when(middle)
    def _():
        for c in hot:
            c.start()

    pick(far_slot, 2, 2 * exp_dev)
    send_rows(1, 0, piece, 0, True)

    def done_send(c):
        if c.is_remote:
            c.wait_send()

    def done_recv(c):
        if c.is_remote:
            c.wait_recv()
        else:
            c.wait()

    for c in weights:
        c.wait()
    for c in sends[0]:
        done_recv(c)
    base_ffn(here, m_ref, recv0, q_ref.at[0], w_ref, d_model, d_ff, base_rows, ret_s.at[0], ret_r.at[0])

    @pl.when(jnp.logical_not(moved))
    def _():
        for h in range(2):
            hb_ref[h] = g_ref[h, slot(0)]

    @pl.when(moved)
    def _():
        hot_tab.wait_recv()
        for c in hot:
            c.wait_recv()

    for c in sends[0]:
        done_send(c)

    def hot_pick(rel):
        @pl.loop(0, exp_dev)
        def _(e):
            mat = pick_matrix(htr_ref[pl.ds(rel * exp_dev + e, 1)], tok_dev)
            for h in range(2):
                m_ref[h, rows_at(rel * hot_dev + e * hot_rows, hot_rows)] = dot(mat, hb_ref[h]).astype(BF16)

    away, here_rows = pl.ds(hot_dev, hot_dev), pl.ds(land, hot_dev)
    hot_pick(1)
    swap = [remote(m_ref.at[h, away], m_ref.at[h, here_rows], swap_s.at[h], swap_r.at[h], here.dev(core=1)) for h in range(2)]
    back = [remote(m_ref.at[h, here_rows], hy_ref.at[h], swap_s.at[2 + h], swap_r.at[2 + h], here.dev(core=1)) for h in range(2)]
    for c in swap:
        c.start()
    hot_pick(0)
    for c in swap:
        c.wait_recv()
    tiles = hot_rows // piece

    @pl.loop(0, exp_dev)
    def _(e):
        @pl.when(e > 0)
        def _():
            for c in load_weights(e, wg_ref, wu_ref, wd_ref, w_ref, w_sem):
                c.wait()

        @pl.loop(0, n_core * tiles)
        def _(k):
            rows = rows_at((k // tiles) * land + e * hot_rows + lax.rem(k, tiles) * piece, piece)
            y1, y2 = gated_mlp(m_ref[0, rows], m_ref[1, rows], w_ref, d_model, d_ff)
            m_ref[0, rows] = y1
            m_ref[1, rows] = y2

    for c in back:
        c.start()

    for c in sends[1]:
        done_recv(c)
        done_send(c)
    x_in = pltpu.make_async_copy(re_ref, m_ref.at[:, pl.ds(n_row, n_row)], x_sem)
    x_in.start()
    x_in.wait()
    base_ffn(here, m_ref, n_row, q_ref.at[1], w_ref, d_model, d_ff, base_rows, ret_s.at[1], ret_r.at[1])

    for h in range(2):
        return_keep(h, m_ref, recv0, q_ref.at[0], ret_s.at[0], piece).wait()
        for j in range(1, n_dst):
            c = return_copy(here, h, j, m_ref, recv0, q_ref.at[0], ret_s.at[0], ret_r.at[0], piece)
            c.wait_send()
            c.wait_recv()
    q_in = pltpu.make_async_copy(q_ref.at[0], m_ref.at[:, pl.ds(recv0, n_row)], x_sem)
    q_in.start()

    for c in swap:
        c.wait_send()
    hy_in = [pltpu.make_async_copy(hy_ref.at[h], m_ref.at[h, away], own_sem.at[h]) for h in range(2)]
    for h in range(2):
        back[h].wait_recv()
        hy_in[h].start()
    for c in hy_in:
        c.wait()
    kinds = n_core * exp_dev

    @pl.loop(0, 2)
    def _(h):
        acc = None
        for k in range(kinds):
            rows = scaled_rows(m_ref[h, pl.ds(k * hot_rows, hot_rows)], htr_ref[kinds + k:kinds + k + 1])
            term = dot(spread_matrix(htr_ref[k:k + 1], tok_dev), rows)
            acc = term if acc is None else acc + term
        hb_ref[h] = acc.astype(BF16)

    sums = [remote(hb_ref.at[h], hs_ref.at[h], sum_s.at[h], sum_r.at[h], here.dev(**{AXES[h][1]: n // 2})) for h in range(2)]

    @pl.when(moved)
    def _():
        for c in sums:
            c.start()

    for c in first + far:
        c.wait_send()

    @pl.when(middle)
    def _():
        for c in hot:
            c.wait_send()

    def load_piece(h, j):
        rows = pl.ds(j * piece, piece)
        return pltpu.make_async_copy(q_ref.at[1, h, rows], g_ref.at[h, rows], load_sem.at[h, j])

    for h in range(2):
        return_keep(h, m_ref, n_row, q_ref.at[1], ret_s.at[1], piece).wait()
        load_piece(h, 0).start()
    for j in range(n_dst - 1, 0, -1):
        for h in range(2):
            return_copy(here, h, j, m_ref, n_row, q_ref.at[1], ret_s.at[1], ret_r.at[1], piece).wait_recv()
            load_piece(h, j).start()
    q_in.wait()
    for h in range(2):
        for j in range(n_dst):
            load_piece(h, j).wait()

    def p_rows(h, s):
        return rows_at((h * n + s) * tok_dev, tok_dev)

    def p_half(h, s, part):
        return pl.ds((h * n + s) * tok_dev + part * half, half)

    def spread(h, s):
        acc = None
        for e, (ref, start) in enumerate(((m_ref, recv0), (g_ref, 0))):
            rows = jnp.concatenate([ref[h, pl.ds(start + j * piece + place(s, n) * base_rows, base_rows)] for j in range(n_dst)], axis=0)
            term = dot(spread_matrix(rx_ref[h, s, pl.ds(2 * e, 1)], tok_dev), scaled_rows(rows, rx_ref[h, s, pl.ds(2 * e + 1, 1)]))
            acc = term if acc is None else acc + term
        return acc

    ring = []

    def send(h, i, s, part, dst, by, start=True):
        c = remote(w_ref.at[p_half(h, s, part)], dst, ring_s.at[h, i], ring_r.at[h, i], here.dev(**{AXES[h][0]: by}))
        if start:
            c.start()
        ring.append(c)
        return c

    tops = []
    for h in range(2):
        w_ref[p_rows(h, far_slot)] = spread(h, far_slot).astype(BF16)
        tops.append(send(h, 0, far_slot, 0, u_ref.at[h, lo], 1, False))
        tops.append(send(h, 1, far_slot, 1, u_ref.at[h, hi], -1, False))

        @pl.when(jnp.logical_not(middle))
        def _():
            tops[2 * h].start()
            tops[2 * h + 1].start()

    last = []
    for s, part, by in ((n - 1, 1, 1), (1, 0, -1)):
        @pl.loop(0, 2)
        def _(h):
            w_ref[p_rows(h, s)] = spread(h, s).astype(BF16)

        for h in range(2):
            last.append(send(h, 2 + part, s, part, v_ref.at[h, 1 - part, (lo, hi)[part]], by))

    def load(ref, h, rows, start):
        c = pltpu.make_async_copy(ref.at[h, rows], m_ref.at[h, pl.ds(start, half)], own_sem.at[h])
        c.start()
        c.wait()
        return m_ref[h, pl.ds(start, half)].astype(F32)

    def add_to(h, s, part, more):
        rows = p_half(h, s, part)
        w_ref[rows] = (w_ref[rows].astype(F32) + more).astype(BF16)

    @pl.when(middle)
    def _():
        for h in range(2):
            sums[h].wait_recv()
            add_to(h, far_slot, 0, load(hs_ref, h, lo, 0))
            tops[2 * h].start()
            add_to(h, far_slot, 1, load(hs_ref, h, hi, 0))
            tops[2 * h + 1].start()

    own_hot = jnp.where(moved, 0.0, 1.0).astype(F32)

    @pl.loop(0, 2)
    def _(h):
        w_ref[p_rows(h, 0)] = (spread(h, 0) + own_hot * hb_ref[h].astype(F32)).astype(BF16)

    out = [pltpu.make_async_copy(w_ref.at[p_rows(h, 0)], p0_ref.at[h], x_sem) for h in range(2)]
    out[0].start()
    out[0].wait()
    out[1].start()
    for h in range(2):
        tops[2 * h].wait_recv()
        add_to(h, n - 1, 0, load(u_ref, h, lo, 0))
        last.append(send(h, 4, n - 1, 0, v_ref.at[h, 0, lo], 1))
        tops[2 * h + 1].wait_recv()
        add_to(h, 1, 1, load(u_ref, h, hi, 0))
        last.append(send(h, 5, 1, 1, v_ref.at[h, 1, hi], -1))

    out[1].wait()
    for c in tabs + back:
        c.wait_send()
    for h in range(2):
        for j in range(1, n_dst):
            return_copy(here, h, j, m_ref, n_row, q_ref.at[1], ret_s.at[1], ret_r.at[1], piece).wait_send()

    @pl.when(moved)
    def _():
        hot_tab.wait_send()
        for c in sums:
            c.wait_send()

    for c in ring:
        c.wait_send()
    for c in last:
        c.wait_recv()


def layer(n, n_core, base_rows, hot_rows, tokens, tx, ht, w_gate, w_up, w_down):
    tok_dev, d_model = tokens.shape
    exp_dev, _, d_ff = w_gate.shape
    dh = d_model // 2
    n_dst = n * n_core
    n_row = n_dst * n * base_rows
    any_ = pl.BlockSpec(memory_space=pl.ANY)
    vm = pl.BlockSpec(memory_space=pltpu.VMEM)
    dma = pltpu.SemaphoreType.DMA
    hbm = lambda *shape: jax.ShapeDtypeStruct(shape, BF16)
    return pl.pallas_call(
        functools.partial(layer_kernel, n, n_core, exp_dev, base_rows, hot_rows),
        out_shape=(hbm(2, tok_dev, dh), hbm(2, 2, tok_dev, dh), hbm(2, n_row, dh), hbm(exp_dev, 2, n_row, dh), hbm(2, tok_dev, dh), hbm(2, tok_dev, dh), hbm(2, exp_dev * hot_rows, dh)),
        in_specs=[any_, vm, vm, any_, any_, any_],
        out_specs=(any_,) * 7,
        scratch_shapes=[
            pltpu.VMEM(tx.shape, F32),
            pltpu.VMEM(ht.shape, F32),
            pltpu.VMEM((2, n * tok_dev, dh), BF16),
            pltpu.VMEM((2, tok_dev, dh), BF16),
            pltpu.VMEM((2, (exp_dev + 1) * n_row + exp_dev * hot_rows, dh), BF16),
            pltpu.VMEM((max(2 * d_model + 2 * d_ff, 2 * n * tok_dev), dh), BF16),
            dma((2,)), dma((4,)), dma((2 * n,)), dma((2 * n,)), dma((2, 6)), dma((2, 6)),
            dma((2, exp_dev, n_dst, 2)), dma((2, exp_dev, n_dst, 2)), dma((2,)), dma((2,)), dma((4,)), dma((4,)), dma,
            dma((exp_dev, 2, n_dst)), dma((exp_dev, 2, n_dst)), dma((2,)), dma((2,)), dma((2, 6)), dma((2, 6)), dma((2, n_dst)),
        ],
        compiler_params=pltpu.CompilerParams(vmem_limit_bytes=VMEM_LIMIT, collective_id=0, has_side_effects=True),
        name='layer',
    )(tokens, tx, ht, w_gate, w_up, w_down)[:2]


def last_sum_kernel(p_ref, v_ref, out_ref):
    dh = p_ref.shape[-1]
    for h in range(2):
        out_ref[:, h * dh:(h + 1) * dh] = (p_ref[h].astype(F32) + v_ref[h, 0].astype(F32) + v_ref[h, 1].astype(F32)).astype(BF16)


def last_sum(p0, v):
    _, tok_dev, dh = p0.shape
    steps = 6
    rows = tok_dev // steps
    return pl.pallas_call(
        last_sum_kernel,
        grid=(steps,),
        out_shape=jax.ShapeDtypeStruct((tok_dev, 2 * dh), BF16),
        in_specs=[pl.BlockSpec((2, rows, dh), lambda i: (0, i, 0)), pl.BlockSpec((2, 2, rows, dh), lambda i: (0, 0, i, 0))],
        out_specs=pl.BlockSpec((rows, 2 * dh), lambda i: (i, 0)),
        name='last_sum',
    )(p0, v)


def solution(mesh):
    grid_y = mesh.shape['ey']
    grid_x = mesh.shape['ex']
    n_core = mesh.shape['core']
    n = grid_x
    n_dev = grid_y * grid_x * n_core
    chip_list = target_chips(grid_y, grid_x)

    def device_body(tokens, expert_ids, gate_prob, w_gate, w_up, w_down):
        tok_dev, top_k = expert_ids.shape
        exp_dev = w_gate.shape[0]
        exp_chip = exp_dev * n_core
        n_exp = exp_dev * n_dev
        n_copy = tok_dev * top_k
        base_rows = 2 * n_copy // (3 * n_exp)
        hot_rows = grid_y * grid_x * base_rows // 2
        core = lax.axis_index('core')
        iy = lax.axis_index('ey')
        ix = lax.axis_index('ex')
        dst_chip = jnp.where(is_moved(iy, ix, n), lax.rem(iy + n // 2, n) * n + lax.rem(ix + n // 2, n), iy * n + ix)

        key = expert_ids.reshape(n_copy) * n_copy + jnp.arange(n_copy, dtype=jnp.int32)
        skey, sgate = lax.sort((key, gate_prob.reshape(n_copy)), num_keys=1, is_stable=False)
        stok = (lax.rem(skey, n_copy) // top_k).astype(F32)
        tab = jnp.stack([stok, sgate])
        lo = dst_chip * exp_chip
        hot_shift = hot_rows * exp_chip // base_rows
        by_block = tab.reshape(2, n_copy // base_rows, base_rows)
        e_id = jnp.arange(n_exp)[None, :, None]
        base = jnp.where(e_id < lo, by_block[:, :n_exp], by_block[:, hot_shift:hot_shift + n_exp])
        hot = lax.dynamic_slice(tab, (0, lo * base_rows), (2, exp_chip * (base_rows + hot_rows)))
        hot = hot.reshape(2, exp_chip, base_rows + hot_rows)
        base = lax.dynamic_update_slice(base, hot[:, :, :base_rows], (0, lo, 0))
        base = base.reshape(2, n, n, n_core, exp_dev, base_rows)
        base = lax.dynamic_slice_in_dim(jnp.concatenate([base, base], axis=1), iy, n, axis=1)
        base = lax.dynamic_slice_in_dim(jnp.concatenate([base, base], axis=2), ix, n, axis=2)
        base = jnp.where(core == 0, base, base[:, :, :, ::-1])
        hot = hot[:, :, base_rows:].reshape(2, n_core, exp_dev, hot_rows)
        hot = jnp.where(core == 0, hot, hot[:, ::-1])
        n_row = n * n_core * base_rows
        tx = jnp.stack([base.transpose(2, 4, 0, 1, 3, 5).reshape(n, exp_dev * 2, n_row), base.transpose(1, 4, 0, 2, 3, 5).reshape(n, exp_dev * 2, n_row)])
        tx = jnp.pad(tx, ((0, 0), (0, 0), (0, 8 - exp_dev * 2), (0, 0)))
        ht = hot.reshape(2 * exp_chip, hot_rows)

        p0, v = layer(n, n_core, base_rows, hot_rows, tokens, tx, ht, w_gate, w_up, w_down)
        return last_sum(p0, v)

    return jax.shard_map(device_body, mesh=mesh, in_specs=(TOKEN_SPEC, TOKEN_SPEC, TOKEN_SPEC, EXPERT_SPEC, EXPERT_SPEC, EXPERT_SPEC), out_specs=TOKEN_SPEC, check_vma=False)
```

```python
import functools

import jax
import jax.numpy as jnp
from jax import lax
from jax.experimental import pallas as pl
from jax.experimental.pallas import tpu as pltpu
from jax.sharding import PartitionSpec as P

TOKEN_SPEC = P(('dp', 'ey', 'ex', 'core'), None)
EXPERT_SPEC = P(('ey', 'ex', 'core'), None, None)
F32 = jnp.float32
BF16 = jnp.bfloat16
VMEM_LIMIT = 62 * 1024 * 1024
MESH = pl.DeviceIdType.MESH
AXES = (('ex', 'ey'), ('ey', 'ex'))


def target_chips(grid_y, grid_x):
    half_y, half_x = grid_y // 2, grid_x // 2
    chip_list = []
    for chip_y in range(grid_y):
        for chip_x in range(grid_x):
            if chip_y == 0 and chip_x < half_x:
                chip_list.append(half_y * grid_x + chip_x + half_x)
            elif chip_y == half_y and chip_x >= half_x:
                chip_list.append(chip_x - half_x)
            else:
                chip_list.append(chip_y * grid_x + chip_x)
    return chip_list


def is_moved(iy, ix, n):
    half = n // 2
    return ((iy == 0) & (ix < half)) | ((iy == half) & (ix >= half))


def row_to_columns(row):
    return jnp.transpose(jnp.broadcast_to(row, (128, row.shape[1])))


def pick_matrix(row, n_tok):
    cols = row_to_columns(row)
    lane = lax.broadcasted_iota(jnp.int32, cols.shape, 1).astype(F32)
    blocks = [(cols == lane + (128.0 * k)).astype(F32).astype(BF16) for k in range(n_tok // 128)]
    return jnp.concatenate(blocks, axis=1)


def spread_matrix(row, n_tok):
    tok = lax.broadcasted_iota(jnp.int32, (n_tok, row.shape[1]), 0).astype(F32)
    return (tok == row).astype(F32).astype(BF16)


def scaled_rows(rows, gate_row):
    cols = row_to_columns(gate_row)
    reps = rows.shape[1] // 128
    return (rows.astype(F32) * jnp.concatenate([cols] * reps, axis=1)).astype(BF16)


def dot(a, b):
    return jnp.dot(a, b, preferred_element_type=F32)


class Here:
    def __init__(self, n, n_core):
        self.n, self.n_core = n, n_core
        self.iy, self.ix, self.ic = (lax.axis_index(a) for a in ('ey', 'ex', 'core'))
        self.at = {'ey': self.iy, 'ex': self.ix, 'core': self.ic}

    def step(self, axis, by):
        size = self.n_core if axis == 'core' else self.n
        return lax.rem(self.at[axis] + (by % size), size)

    def dev(self, **by):
        return {axis: self.step(axis, k) for axis, k in by.items()}

    def moved(self):
        return is_moved(self.iy, self.ix, self.n)

    def middle(self):
        return is_moved(self.iy, self.step('ex', self.n // 2), self.n)

    def barrier(self):
        sem = pltpu.get_barrier_semaphore()
        peers = [self.dev(**{axis: k, 'core': c}) for axis in ('ey', 'ex') for k in range(1, self.n) for c in range(self.n_core)]
        peers += [self.dev(core=1), self.dev(ey=self.n // 2, ex=self.n // 2)]
        for peer in peers:
            pl.semaphore_signal(sem, inc=1, device_id=peer, device_id_type=MESH)
        pl.semaphore_wait(sem, len(peers))


def remote(src, dst, send_sem, recv_sem, dev):
    return pltpu.make_async_remote_copy(src_ref=src, dst_ref=dst, send_sem=send_sem, recv_sem=recv_sem, device_id=dev, device_id_type=MESH)


def rows_at(start, size):
    return pl.ds(pl.multiple_of(start, size), size)


def load_weights(e, wg_ref, wu_ref, wd_ref, w_ref, sem):
    d_model, d_ff = wg_ref.shape[1:]
    dh = d_model // 2
    copies = [
        pltpu.make_async_copy(wg_ref.at[e], w_ref.at[pl.ds(0, d_model)], sem.at[0]),
        pltpu.make_async_copy(wu_ref.at[e], w_ref.at[pl.ds(d_model, d_model)], sem.at[1]),
        pltpu.make_async_copy(wd_ref.at[e, :, pl.ds(0, dh)], w_ref.at[pl.ds(2 * d_model, d_ff)], sem.at[2]),
        pltpu.make_async_copy(wd_ref.at[e, :, pl.ds(dh, dh)], w_ref.at[pl.ds(2 * d_model + d_ff, d_ff)], sem.at[3]),
    ]
    for c in copies:
        c.start()
    return copies


def gated_mlp(x1, x2, w_ref, d_model, d_ff):
    dh = d_model // 2
    gate = dot(x1, w_ref[0:dh]) + dot(x2, w_ref[dh:d_model])
    up = dot(x1, w_ref[d_model:d_model + dh]) + dot(x2, w_ref[d_model + dh:2 * d_model])
    hidden = (jax.nn.silu(gate) * up).astype(BF16)
    y1 = dot(hidden, w_ref[2 * d_model:2 * d_model + d_ff]).astype(BF16)
    y2 = dot(hidden, w_ref[2 * d_model + d_ff:2 * d_model + 2 * d_ff]).astype(BF16)
    return y1, y2


def place(off, n):
    if isinstance(off, int):
        return off if off < n // 2 else (n - 1 if off == n // 2 else off - 1)
    return jnp.where(off < n // 2, off, jnp.where(off == n // 2, n - 1, off - 1))


def return_copy(here, h, j, src, start, dst, s_sem, r_sem, piece):
    axis = AXES[h][1]
    size = here.n_core
    dev = here.dev(**{axis: here.n - j // size, 'core': j % size})
    return remote(src.at[h, rows_at(start + j * piece, piece)], dst.at[h, rows_at(j * piece, piece)], s_sem.at[h, j], r_sem.at[h, j], dev)


def return_keep(h, src, start, dst, s_sem, piece):
    return pltpu.make_async_copy(src.at[h, pl.ds(start, piece)], dst.at[h, pl.ds(0, piece)], s_sem.at[h, 0])


def base_ffn(here, x_ref, start, dst_ref, w_ref, d_model, d_ff, base_rows, s_sem, r_sem):
    n, n_core = here.n, here.n_core
    piece = n * base_rows

    @pl.loop(0, n * n_core)
    def _(t):
        dc, dy = t // n, lax.rem(t + 1, n)
        j = dy * n_core + dc
        rows1 = rows_at(start + j * piece, piece)
        rows2 = [None] * n
        for dx in range(n):
            rows2[place(dx, n)] = rows_at(start + (dx * n_core + dc) * piece + place(dy, n) * base_rows, base_rows)
        x2 = jnp.concatenate([x_ref[1, r] for r in rows2], axis=0)
        y1, y2 = gated_mlp(x_ref[0, rows1], x2, w_ref, d_model, d_ff)
        x_ref[0, rows1] = y1
        for i in range(n):
            x_ref[1, rows2[i]] = y2[i * base_rows:(i + 1) * base_rows]

        @pl.when(j > 0)
        def _():
            return_copy(here, 0, j, x_ref, start, dst_ref, s_sem, r_sem, piece).start()

        @pl.when(j == 0)
        def _():
            return_keep(0, x_ref, start, dst_ref, s_sem, piece).start()

        def part(dx):
            jx = dx * n_core + dc
            first_row = place(dy, n) * base_rows
            dev = here.dev(**{AXES[1][1]: n - dx, 'core': dc})
            src = x_ref.at[1, rows_at(start + jx * piece + first_row, base_rows)]
            return remote(src, dst_ref.at[1, rows_at(jx * piece + first_row, base_rows)], s_sem.at[1, jx], r_sem.at[1, jx], dev)

        for dx in range(n - 1, 0, -1):
            part(dx).start()

        @pl.when(dc > 0)
        def _():
            part(0).start()

        @pl.when((dc == 0) & (dy == 0))
        def _():
            return_keep(1, x_ref, start, dst_ref, s_sem, piece).start()


def layer_kernel(n, n_core, exp_dev, base_rows, hot_rows, tok_ref, tx_ref, ht_ref, wg_ref, wu_ref, wd_ref,
                 p0_ref, v_ref, re_ref, q_ref, hs_ref, hy_ref,
                 rx_ref, htr_ref, g_ref, hb_ref, m_ref, w_ref,
                 own_sem, w_sem, tab_s, tab_r, g_s, g_r, d_s, d_r, hot_s, hot_r, swap_s, swap_r, x_sem, ret_s, ret_r, sum_s, sum_r, ring_s, ring_r, load_sem, free_sem):
    here = Here(n, n_core)
    tok_dev, d_model = tok_ref.shape
    d_ff = wg_ref.shape[2]
    dh = d_model // 2
    half = tok_dev // 2
    n_dst = n * n_core
    piece = n * base_rows
    n_row = n_dst * piece
    hot_dev = exp_dev * hot_rows
    land = exp_dev * n_row
    recv0 = land + hot_dev
    far_slot = n // 2
    lo, hi = pl.ds(0, half), pl.ds(half, half)

    def slot(s, part=None):
        return pl.ds(s * tok_dev, tok_dev) if part is None else pl.ds(s * tok_dev + part * half, half)

    own = [pltpu.make_async_copy(tok_ref.at[:, pl.ds(h * dh, dh)], g_ref.at[h, slot(0)], own_sem.at[h]) for h in range(2)]
    for c in own:
        c.start()
    here.barrier()

    tabs = []
    for h in range(2):
        rx_ref[h, 0] = tx_ref[h, 0]
        for k in range(1, n):
            c = remote(tx_ref.at[h, k], rx_ref.at[h, k], tab_s.at[h * n + k], tab_r.at[h * n + k], here.dev(**{AXES[h][0]: k}))
            c.start()
            tabs.append(c)
    moved = here.moved()
    middle = here.middle()
    hot_tab = remote(ht_ref, htr_ref, tab_s.at[0], tab_r.at[0], here.dev(ey=n // 2, ex=n // 2))

    @pl.when(moved)
    def _():
        hot_tab.start()

    @pl.when(jnp.logical_not(moved))
    def _():
        htr_ref[...] = ht_ref[...]

    first = []
    for h in range(2):
        own[h].wait()
        axis = AXES[h][0]
        for i, (s, part, by) in enumerate(((1, 0, 1), (n - 1, 1, -1), (1, 1, 1), (n - 1, 0, -1))):
            c = remote(g_ref.at[h, slot(0, part)], g_ref.at[h, slot(s, part)], g_s.at[h, i], g_r.at[h, i], here.dev(**{axis: by}))
            c.start()
            first.append(c)
    weights = load_weights(0, wg_ref, wu_ref, wd_ref, w_ref, w_sem)
    for c in tabs:
        c.wait_recv()

    def pick(s, start, stop):
        @pl.loop(start, stop)
        def _(m):
            e, h = m // 2, lax.rem(m, 2)
            mat = pick_matrix(rx_ref[h, s, pl.ds(2 * e, 1)], tok_dev)
            picked = dot(mat, g_ref[h, slot(s)]).astype(BF16)
            for j in range(n_dst):
                m_ref[h, rows_at(e * n_row + j * piece + place(s, n) * base_rows, base_rows)] = picked[j * base_rows:(j + 1) * base_rows]

    sends = [[], []]

    def send_rows(e, first_row, size, i, keep):
        for j in range(n_dst - 1, -1 if keep else 0, -1):
            for h in range(2):
                if j:
                    src = m_ref.at[h, pl.ds(e * n_row + j * piece + first_row, size)]
                    dst = m_ref.at[h, pl.ds(recv0 + j * piece + first_row, size)] if e == 0 else re_ref.at[h, pl.ds(j * piece + first_row, size)]
                    c = remote(src, dst, d_s.at[h, e, j, i], d_r.at[h, e, j, i], here.dev(**{AXES[h][1]: j // n_core, 'core': j % n_core}))
                else:
                    dst = m_ref.at[h, pl.ds(recv0, piece)] if e == 0 else re_ref.at[h, pl.ds(0, piece)]
                    c = pltpu.make_async_copy(m_ref.at[h, pl.ds(e * n_row, piece)], dst, d_s.at[h, e, j, i])
                c.start()
                sends[e].append(c)

    pick(0, 0, 2 * exp_dev)
    far = []
    for i, (s, part, by) in enumerate(((1, 0, 1), (n - 1, 1, -1))):
        for h in range(2):
            first[h * 4 + i].wait_recv()
            c = remote(g_ref.at[h, slot(s, part)], g_ref.at[h, slot(far_slot, part)], g_s.at[h, 4 + i], g_r.at[h, 4 + i], here.dev(**{AXES[h][0]: by}))
            c.start()
            far.append(c)
    for i, s in enumerate((1, n - 1)):
        for h in range(2):
            first[h * 4 + 2 + i].wait_recv()
        pick(s, 0, 2 * exp_dev)
    send_rows(0, 0, piece - base_rows, 0, False)
    for c in far:
        c.wait_recv()
    pick(far_slot, 0, 2)
    send_rows(0, piece - base_rows, base_rows, 1, True)

    hot = [remote(g_ref.at[h, slot(far_slot)], hb_ref.at[h], hot_s.at[h], hot_r.at[h], here.dev(**{AXES[h][1]: n // 2})) for h in range(2)]

    @pl.when(middle)
    def _():
        for c in hot:
            c.start()

    pick(far_slot, 2, 2 * exp_dev)
    send_rows(1, 0, piece, 0, True)

    def done_send(c):
        if c.is_remote:
            c.wait_send()

    def done_recv(c):
        if c.is_remote:
            c.wait_recv()
        else:
            c.wait()

    for c in weights:
        c.wait()
    for c in sends[0]:
        done_recv(c)
    base_ffn(here, m_ref, recv0, q_ref.at[0], w_ref, d_model, d_ff, base_rows, ret_s.at[0], ret_r.at[0])

    @pl.when(jnp.logical_not(moved))
    def _():
        for h in range(2):
            hb_ref[h] = g_ref[h, slot(0)]

    @pl.when(moved)
    def _():
        hot_tab.wait_recv()
        for c in hot:
            c.wait_recv()

    for c in sends[0]:
        done_send(c)

    def hot_pick(rel):
        @pl.loop(0, exp_dev)
        def _(e):
            mat = pick_matrix(htr_ref[pl.ds(rel * exp_dev + e, 1)], tok_dev)
            for h in range(2):
                m_ref[h, rows_at(rel * hot_dev + e * hot_rows, hot_rows)] = dot(mat, hb_ref[h]).astype(BF16)

    away, here_rows = pl.ds(hot_dev, hot_dev), pl.ds(land, hot_dev)
    hot_pick(1)
    swap = [remote(m_ref.at[h, away], m_ref.at[h, here_rows], swap_s.at[h], swap_r.at[h], here.dev(core=1)) for h in range(2)]
    back = [remote(m_ref.at[h, here_rows], hy_ref.at[h], swap_s.at[2 + h], swap_r.at[2 + h], here.dev(core=1)) for h in range(2)]
    for c in swap:
        c.start()
    hot_pick(0)
    for c in swap:
        c.wait_recv()
    tiles = hot_rows // piece

    @pl.loop(0, exp_dev)
    def _(e):
        @pl.when(e > 0)
        def _():
            for c in load_weights(e, wg_ref, wu_ref, wd_ref, w_ref, w_sem):
                c.wait()

        @pl.loop(0, n_core * tiles)
        def _(k):
            rows = rows_at((k // tiles) * land + e * hot_rows + lax.rem(k, tiles) * piece, piece)
            y1, y2 = gated_mlp(m_ref[0, rows], m_ref[1, rows], w_ref, d_model, d_ff)
            m_ref[0, rows] = y1
            m_ref[1, rows] = y2

    for c in back:
        c.start()

    for c in sends[1]:
        done_recv(c)
        done_send(c)
    x_in = pltpu.make_async_copy(re_ref, m_ref.at[:, pl.ds(n_row, n_row)], x_sem)
    x_in.start()
    x_in.wait()
    base_ffn(here, m_ref, n_row, q_ref.at[1], w_ref, d_model, d_ff, base_rows, ret_s.at[1], ret_r.at[1])

    for h in range(2):
        return_keep(h, m_ref, recv0, q_ref.at[0], ret_s.at[0], piece).wait()
        for j in range(1, n_dst):
            c = return_copy(here, h, j, m_ref, recv0, q_ref.at[0], ret_s.at[0], ret_r.at[0], piece)
            c.wait_send()
            c.wait_recv()
    q_in = pltpu.make_async_copy(q_ref.at[0], m_ref.at[:, pl.ds(recv0, n_row)], x_sem)
    q_in.start()

    for c in swap:
        c.wait_send()
    hy_in = [pltpu.make_async_copy(hy_ref.at[h], m_ref.at[h, away], own_sem.at[h]) for h in range(2)]
    for h in range(2):
        back[h].wait_recv()
        hy_in[h].start()
    for c in hy_in:
        c.wait()
    kinds = n_core * exp_dev

    @pl.loop(0, 2)
    def _(h):
        acc = None
        for k in range(kinds):
            rows = scaled_rows(m_ref[h, pl.ds(k * hot_rows, hot_rows)], htr_ref[kinds + k:kinds + k + 1])
            term = dot(spread_matrix(htr_ref[k:k + 1], tok_dev), rows)
            acc = term if acc is None else acc + term
        hb_ref[h] = acc.astype(BF16)

    sums = [remote(hb_ref.at[h], hs_ref.at[h], sum_s.at[h], sum_r.at[h], here.dev(**{AXES[h][1]: n // 2})) for h in range(2)]

    @pl.when(moved)
    def _():
        for c in sums:
            c.start()

    for h in range(2):
        for i, by in enumerate((-1, 1)):
            pl.semaphore_signal(free_sem.at[h, i], inc=1, device_id=here.dev(**{AXES[h][0]: by}), device_id_type=MESH)

    for c in first + far:
        c.wait_send()

    @pl.when(middle)
    def _():
        for c in hot:
            c.wait_send()

    def load_piece(h, j):
        rows = pl.ds(j * piece, piece)
        return pltpu.make_async_copy(q_ref.at[1, h, rows], g_ref.at[h, rows], load_sem.at[h, j])

    for h in range(2):
        return_keep(h, m_ref, n_row, q_ref.at[1], ret_s.at[1], piece).wait()
        load_piece(h, 0).start()
    for j in range(n_dst - 1, 0, -1):
        for h in range(2):
            return_copy(here, h, j, m_ref, n_row, q_ref.at[1], ret_s.at[1], ret_r.at[1], piece).wait_recv()
            load_piece(h, j).start()
    q_in.wait()
    for h in range(2):
        for j in range(n_dst):
            load_piece(h, j).wait()

    def p_rows(h, s):
        return rows_at((h * n + s) * tok_dev, tok_dev)

    quarter = half // 2

    def quarters(part):
        return [pl.ds((2 * part + q) * quarter, quarter) for q in range(2)]

    def p_part(h, s, part):
        return pl.ds((h * n + s) * tok_dev + part.start, part.size)

    def spread(h, s):
        acc = None
        for e, (ref, start) in enumerate(((m_ref, recv0), (g_ref, 0))):
            rows = jnp.concatenate([ref[h, pl.ds(start + j * piece + place(s, n) * base_rows, base_rows)] for j in range(n_dst)], axis=0)
            term = dot(spread_matrix(rx_ref[h, s, pl.ds(2 * e, 1)], tok_dev), scaled_rows(rows, rx_ref[h, s, pl.ds(2 * e + 1, 1)]))
            acc = term if acc is None else acc + term
        return acc

    ring = []

    def send(h, i, s, part, dst, by, start=True):
        c = remote(w_ref.at[p_part(h, s, part)], dst, ring_s.at[h, i], ring_r.at[h, i], here.dev(**{AXES[h][0]: by}))
        if start:
            c.start()
        ring.append(c)
        return c

    tops = [[], []]
    for h in range(2):
        w_ref[p_rows(h, far_slot)] = spread(h, far_slot).astype(BF16)
        for q in range(2):
            tops[h].append(send(h, q, far_slot, quarters(0)[q], m_ref.at[h, quarters(0)[q]], 1, False))
            tops[h].append(send(h, 2 + q, far_slot, quarters(1)[q], m_ref.at[h, quarters(1)[q]], -1, False))

        for i in range(2):
            pl.semaphore_wait(free_sem.at[h, i], 1)

        @pl.when(jnp.logical_not(middle))
        def _():
            for c in tops[h]:
                c.start()

    last = []
    for s, part, by in ((n - 1, 1, 1), (1, 0, -1)):
        @pl.loop(0, 2)
        def _(h):
            w_ref[p_rows(h, s)] = spread(h, s).astype(BF16)

        for h in range(2):
            last.append(send(h, 4 + part, s, (lo, hi)[part], v_ref.at[h, 1 - part, (lo, hi)[part]], by))

    def add_to(h, s, part, start=0):
        rows = p_part(h, s, part)
        more = m_ref[h, pl.ds(start + part.start, part.size)]
        w_ref[rows] = (w_ref[rows].astype(F32) + more.astype(F32)).astype(BF16)

    @pl.when(middle)
    def _():
        loads = [pltpu.make_async_copy(hs_ref.at[h], m_ref.at[h, pl.ds(hot_dev, tok_dev)], own_sem.at[h]) for h in range(2)]
        for h in range(2):
            sums[h].wait_recv()
            loads[h].start()
        for h in range(2):
            loads[h].wait()
            for q in range(2):
                add_to(h, far_slot, quarters(0)[q], hot_dev)
                tops[h][2 * q].start()
                add_to(h, far_slot, quarters(1)[q], hot_dev)
                tops[h][2 * q + 1].start()

    own_hot = jnp.where(moved, 0.0, 1.0).astype(F32)

    @pl.loop(0, 2)
    def _(h):
        w_ref[p_rows(h, 0)] = (spread(h, 0) + own_hot * hb_ref[h].astype(F32)).astype(BF16)

    out = [pltpu.make_async_copy(w_ref.at[p_rows(h, 0)], p0_ref.at[h], own_sem.at[h]) for h in range(2)]
    for c in out:
        c.start()
    for q in range(2):
        for h in range(2):
            tops[h][2 * q].wait_recv()
            add_to(h, n - 1, quarters(0)[q])
            last.append(send(h, 6 + q, n - 1, quarters(0)[q], v_ref.at[h, 0, quarters(0)[q]], 1))
            tops[h][2 * q + 1].wait_recv()
            add_to(h, 1, quarters(1)[q])
            last.append(send(h, 8 + q, 1, quarters(1)[q], v_ref.at[h, 1, quarters(1)[q]], -1))

    for c in out:
        c.wait()
    for c in tabs + back:
        c.wait_send()
    for h in range(2):
        for j in range(1, n_dst):
            return_copy(here, h, j, m_ref, n_row, q_ref.at[1], ret_s.at[1], ret_r.at[1], piece).wait_send()

    @pl.when(moved)
    def _():
        hot_tab.wait_send()
        for c in sums:
            c.wait_send()

    for c in ring:
        c.wait_send()
    for c in last:
        c.wait_recv()


def layer(n, n_core, base_rows, hot_rows, tokens, tx, ht, w_gate, w_up, w_down):
    tok_dev, d_model = tokens.shape
    exp_dev, _, d_ff = w_gate.shape
    dh = d_model // 2
    n_dst = n * n_core
    n_row = n_dst * n * base_rows
    any_ = pl.BlockSpec(memory_space=pl.ANY)
    vm = pl.BlockSpec(memory_space=pltpu.VMEM)
    dma = pltpu.SemaphoreType.DMA
    hbm = lambda *shape: jax.ShapeDtypeStruct(shape, BF16)
    return pl.pallas_call(
        functools.partial(layer_kernel, n, n_core, exp_dev, base_rows, hot_rows),
        out_shape=(hbm(2, tok_dev, dh), hbm(2, 2, tok_dev, dh), hbm(2, n_row, dh), hbm(exp_dev, 2, n_row, dh), hbm(2, tok_dev, dh), hbm(2, exp_dev * hot_rows, dh)),
        in_specs=[any_, vm, vm, any_, any_, any_],
        out_specs=(any_,) * 6,
        scratch_shapes=[
            pltpu.VMEM(tx.shape, F32),
            pltpu.VMEM(ht.shape, F32),
            pltpu.VMEM((2, n * tok_dev, dh), BF16),
            pltpu.VMEM((2, tok_dev, dh), BF16),
            pltpu.VMEM((2, (exp_dev + 1) * n_row + exp_dev * hot_rows, dh), BF16),
            pltpu.VMEM((max(2 * d_model + 2 * d_ff, 2 * n * tok_dev), dh), BF16),
            dma((2,)), dma((4,)), dma((2 * n,)), dma((2 * n,)), dma((2, 6)), dma((2, 6)),
            dma((2, exp_dev, n_dst, 2)), dma((2, exp_dev, n_dst, 2)), dma((2,)), dma((2,)), dma((4,)), dma((4,)), dma,
            dma((exp_dev, 2, n_dst)), dma((exp_dev, 2, n_dst)), dma((2,)), dma((2,)), dma((2, 10)), dma((2, 10)), dma((2, n_dst)), pltpu.SemaphoreType.REGULAR((2, 2)),
        ],
        compiler_params=pltpu.CompilerParams(vmem_limit_bytes=VMEM_LIMIT, collective_id=0, has_side_effects=True),
        name='layer',
    )(tokens, tx, ht, w_gate, w_up, w_down)[:2]


def last_sum_kernel(p_ref, v_ref, out_ref):
    dh = p_ref.shape[-1]
    for h in range(2):
        out_ref[:, h * dh:(h + 1) * dh] = (p_ref[h].astype(F32) + v_ref[h, 0].astype(F32) + v_ref[h, 1].astype(F32)).astype(BF16)


def last_sum(p0, v):
    _, tok_dev, dh = p0.shape
    steps = 6
    rows = tok_dev // steps
    return pl.pallas_call(
        last_sum_kernel,
        grid=(steps,),
        out_shape=jax.ShapeDtypeStruct((tok_dev, 2 * dh), BF16),
        in_specs=[pl.BlockSpec((2, rows, dh), lambda i: (0, i, 0)), pl.BlockSpec((2, 2, rows, dh), lambda i: (0, 0, i, 0))],
        out_specs=pl.BlockSpec((rows, 2 * dh), lambda i: (i, 0)),
        name='last_sum',
    )(p0, v)


def solution(mesh):
    grid_y = mesh.shape['ey']
    grid_x = mesh.shape['ex']
    n_core = mesh.shape['core']
    n = grid_x
    n_dev = grid_y * grid_x * n_core
    chip_list = target_chips(grid_y, grid_x)

    def device_body(tokens, expert_ids, gate_prob, w_gate, w_up, w_down):
        tok_dev, top_k = expert_ids.shape
        exp_dev = w_gate.shape[0]
        exp_chip = exp_dev * n_core
        n_exp = exp_dev * n_dev
        n_copy = tok_dev * top_k
        base_rows = 2 * n_copy // (3 * n_exp)
        hot_rows = grid_y * grid_x * base_rows // 2
        core = lax.axis_index('core')
        iy = lax.axis_index('ey')
        ix = lax.axis_index('ex')
        dst_chip = jnp.where(is_moved(iy, ix, n), lax.rem(iy + n // 2, n) * n + lax.rem(ix + n // 2, n), iy * n + ix)

        key = expert_ids.reshape(n_copy) * n_copy + jnp.arange(n_copy, dtype=jnp.int32)
        skey, sgate = lax.sort((key, gate_prob.reshape(n_copy)), num_keys=1, is_stable=False)
        stok = (lax.rem(skey, n_copy) // top_k).astype(F32)
        tab = jnp.stack([stok, sgate])
        lo = dst_chip * exp_chip
        hot_shift = hot_rows * exp_chip // base_rows
        by_block = tab.reshape(2, n_copy // base_rows, base_rows)
        e_id = jnp.arange(n_exp)[None, :, None]
        base = jnp.where(e_id < lo, by_block[:, :n_exp], by_block[:, hot_shift:hot_shift + n_exp])
        hot = lax.dynamic_slice(tab, (0, lo * base_rows), (2, exp_chip * (base_rows + hot_rows)))
        hot = hot.reshape(2, exp_chip, base_rows + hot_rows)
        base = lax.dynamic_update_slice(base, hot[:, :, :base_rows], (0, lo, 0))
        base = base.reshape(2, n, n, n_core, exp_dev, base_rows)
        base = lax.dynamic_slice_in_dim(jnp.concatenate([base, base], axis=1), iy, n, axis=1)
        base = lax.dynamic_slice_in_dim(jnp.concatenate([base, base], axis=2), ix, n, axis=2)
        base = jnp.where(core == 0, base, base[:, :, :, ::-1])
        hot = hot[:, :, base_rows:].reshape(2, n_core, exp_dev, hot_rows)
        hot = jnp.where(core == 0, hot, hot[:, ::-1])
        n_row = n * n_core * base_rows
        tx = jnp.stack([base.transpose(2, 4, 0, 1, 3, 5).reshape(n, exp_dev * 2, n_row), base.transpose(1, 4, 0, 2, 3, 5).reshape(n, exp_dev * 2, n_row)])
        tx = jnp.pad(tx, ((0, 0), (0, 0), (0, 8 - exp_dev * 2), (0, 0)))
        ht = hot.reshape(2 * exp_chip, hot_rows)

        p0, v = layer(n, n_core, base_rows, hot_rows, tokens, tx, ht, w_gate, w_up, w_down)
        return last_sum(p0, v)

    return jax.shard_map(device_body, mesh=mesh, in_specs=(TOKEN_SPEC, TOKEN_SPEC, TOKEN_SPEC, EXPERT_SPEC, EXPERT_SPEC, EXPERT_SPEC), out_specs=TOKEN_SPEC, check_vma=False)
```

```python
import functools

import jax
import jax.numpy as jnp
from jax import lax
from jax.experimental import pallas as pl
from jax.experimental.pallas import tpu as pltpu
from jax.sharding import PartitionSpec as P

TOKEN_SPEC = P(('dp', 'ey', 'ex', 'core'), None)
EXPERT_SPEC = P(('ey', 'ex', 'core'), None, None)
F32 = jnp.float32
BF16 = jnp.bfloat16
VMEM_LIMIT = 62 * 1024 * 1024
MESH = pl.DeviceIdType.MESH
AXES = (('ex', 'ey'), ('ey', 'ex'))


def target_chips(grid_y, grid_x):
    half_y, half_x = grid_y // 2, grid_x // 2
    chip_list = []
    for chip_y in range(grid_y):
        for chip_x in range(grid_x):
            if chip_y == 0 and chip_x < half_x:
                chip_list.append(half_y * grid_x + chip_x + half_x)
            elif chip_y == half_y and chip_x >= half_x:
                chip_list.append(chip_x - half_x)
            else:
                chip_list.append(chip_y * grid_x + chip_x)
    return chip_list


def is_moved(iy, ix, n):
    half = n // 2
    return ((iy == 0) & (ix < half)) | ((iy == half) & (ix >= half))


def row_to_columns(row):
    return jnp.transpose(jnp.broadcast_to(row, (128, row.shape[1])))


def pick_matrix(row, n_tok):
    cols = row_to_columns(row)
    lane = lax.broadcasted_iota(jnp.int32, cols.shape, 1).astype(F32)
    blocks = [(cols == lane + (128.0 * k)).astype(F32).astype(BF16) for k in range(n_tok // 128)]
    return jnp.concatenate(blocks, axis=1)


def spread_matrix(row, n_tok):
    tok = lax.broadcasted_iota(jnp.int32, (n_tok, row.shape[1]), 0).astype(F32)
    return (tok == row).astype(F32).astype(BF16)


def scaled_rows(rows, gate_row):
    cols = row_to_columns(gate_row)
    reps = rows.shape[1] // 128
    return (rows.astype(F32) * jnp.concatenate([cols] * reps, axis=1)).astype(BF16)


def dot(a, b):
    return jnp.dot(a, b, preferred_element_type=F32)


class Here:
    def __init__(self, n, n_core):
        self.n, self.n_core = n, n_core
        self.iy, self.ix, self.ic = (lax.axis_index(a) for a in ('ey', 'ex', 'core'))
        self.at = {'ey': self.iy, 'ex': self.ix, 'core': self.ic}

    def step(self, axis, by):
        size = self.n_core if axis == 'core' else self.n
        return lax.rem(self.at[axis] + (by % size), size)

    def dev(self, **by):
        return {axis: self.step(axis, k) for axis, k in by.items()}

    def moved(self):
        return is_moved(self.iy, self.ix, self.n)

    def middle(self):
        return is_moved(self.iy, self.step('ex', self.n // 2), self.n)

    def barrier(self):
        sem = pltpu.get_barrier_semaphore()
        peers = [self.dev(**{axis: k, 'core': c}) for axis in ('ey', 'ex') for k in range(1, self.n) for c in range(self.n_core)]
        peers += [self.dev(core=1), self.dev(ey=self.n // 2, ex=self.n // 2)]
        for peer in peers:
            pl.semaphore_signal(sem, inc=1, device_id=peer, device_id_type=MESH)
        pl.semaphore_wait(sem, len(peers))


def remote(src, dst, send_sem, recv_sem, dev):
    return pltpu.make_async_remote_copy(src_ref=src, dst_ref=dst, send_sem=send_sem, recv_sem=recv_sem, device_id=dev, device_id_type=MESH)


def rows_at(start, size):
    return pl.ds(pl.multiple_of(start, size), size)


def load_weights(e, wg_ref, wu_ref, wd_ref, w_ref, sem):
    d_model, d_ff = wg_ref.shape[1:]
    dh = d_model // 2
    copies = [
        pltpu.make_async_copy(wg_ref.at[e], w_ref.at[pl.ds(0, d_model)], sem.at[0]),
        pltpu.make_async_copy(wu_ref.at[e], w_ref.at[pl.ds(d_model, d_model)], sem.at[1]),
        pltpu.make_async_copy(wd_ref.at[e, :, pl.ds(0, dh)], w_ref.at[pl.ds(2 * d_model, d_ff)], sem.at[2]),
        pltpu.make_async_copy(wd_ref.at[e, :, pl.ds(dh, dh)], w_ref.at[pl.ds(2 * d_model + d_ff, d_ff)], sem.at[3]),
    ]
    for c in copies:
        c.start()
    return copies


def gated_mlp(x1, x2, w_ref, d_model, d_ff):
    dh = d_model // 2
    gate = dot(x1, w_ref[0:dh]) + dot(x2, w_ref[dh:d_model])
    up = dot(x1, w_ref[d_model:d_model + dh]) + dot(x2, w_ref[d_model + dh:2 * d_model])
    hidden = (jax.nn.silu(gate) * up).astype(BF16)
    y1 = dot(hidden, w_ref[2 * d_model:2 * d_model + d_ff]).astype(BF16)
    y2 = dot(hidden, w_ref[2 * d_model + d_ff:2 * d_model + 2 * d_ff]).astype(BF16)
    return y1, y2


def place(off, n):
    if isinstance(off, int):
        return off if off < n // 2 else (n - 1 if off == n // 2 else off - 1)
    return jnp.where(off < n // 2, off, jnp.where(off == n // 2, n - 1, off - 1))


def return_copy(here, h, j, src, start, dst, s_sem, r_sem, piece):
    axis = AXES[h][1]
    size = here.n_core
    dev = here.dev(**{axis: here.n - j // size, 'core': j % size})
    return remote(src.at[h, rows_at(start + j * piece, piece)], dst.at[h, rows_at(j * piece, piece)], s_sem.at[h, j], r_sem.at[h, j], dev)


def return_keep(h, src, start, dst, s_sem, piece):
    return pltpu.make_async_copy(src.at[h, pl.ds(start, piece)], dst.at[h, pl.ds(0, piece)], s_sem.at[h, 0])


def base_ffn(here, x_ref, start, dst_ref, w_ref, d_model, d_ff, base_rows, s_sem, r_sem):
    n, n_core = here.n, here.n_core
    piece = n * base_rows

    @pl.loop(0, n * n_core)
    def _(t):
        dc, dy = t // n, lax.rem(t + 1, n)
        j = dy * n_core + dc
        rows1 = rows_at(start + j * piece, piece)
        rows2 = [None] * n
        for dx in range(n):
            rows2[place(dx, n)] = rows_at(start + (dx * n_core + dc) * piece + place(dy, n) * base_rows, base_rows)
        x2 = jnp.concatenate([x_ref[1, r] for r in rows2], axis=0)
        y1, y2 = gated_mlp(x_ref[0, rows1], x2, w_ref, d_model, d_ff)
        x_ref[0, rows1] = y1
        for i in range(n):
            x_ref[1, rows2[i]] = y2[i * base_rows:(i + 1) * base_rows]

        @pl.when(j > 0)
        def _():
            return_copy(here, 0, j, x_ref, start, dst_ref, s_sem, r_sem, piece).start()

        @pl.when(j == 0)
        def _():
            return_keep(0, x_ref, start, dst_ref, s_sem, piece).start()

        def part(dx):
            jx = dx * n_core + dc
            first_row = place(dy, n) * base_rows
            dev = here.dev(**{AXES[1][1]: n - dx, 'core': dc})
            src = x_ref.at[1, rows_at(start + jx * piece + first_row, base_rows)]
            return remote(src, dst_ref.at[1, rows_at(jx * piece + first_row, base_rows)], s_sem.at[1, jx], r_sem.at[1, jx], dev)

        for dx in range(n - 1, 0, -1):
            part(dx).start()

        @pl.when(dc > 0)
        def _():
            part(0).start()

        @pl.when((dc == 0) & (dy == 0))
        def _():
            return_keep(1, x_ref, start, dst_ref, s_sem, piece).start()


def layer_kernel(n, n_core, exp_dev, base_rows, hot_rows, tok_ref, tx_ref, ht_ref, wg_ref, wu_ref, wd_ref,
                 p0_ref, v_ref, re_ref, q_ref, hs_ref, hy_ref,
                 rx_ref, htr_ref, g_ref, hb_ref, m_ref, w_ref,
                 own_sem, w_sem, tab_s, tab_r, g_s, g_r, d_s, d_r, hot_s, hot_r, swap_s, swap_r, x_sem, ret_s, ret_r, sum_s, sum_r, ring_s, ring_r, load_sem, free_sem):
    here = Here(n, n_core)
    tok_dev, d_model = tok_ref.shape
    d_ff = wg_ref.shape[2]
    dh = d_model // 2
    half = tok_dev // 2
    n_dst = n * n_core
    piece = n * base_rows
    n_row = n_dst * piece
    hot_dev = exp_dev * hot_rows
    land = exp_dev * n_row
    recv0 = land + hot_dev
    far_slot = n // 2
    lo, hi = pl.ds(0, half), pl.ds(half, half)

    def slot(s, part=None):
        return pl.ds(s * tok_dev, tok_dev) if part is None else pl.ds(s * tok_dev + part * half, half)

    own = [pltpu.make_async_copy(tok_ref.at[:, pl.ds(h * dh, dh)], g_ref.at[h, slot(0)], own_sem.at[h]) for h in range(2)]
    for c in own:
        c.start()
    here.barrier()

    tabs = []
    for h in range(2):
        rx_ref[h, 0] = tx_ref[h, 0]
        for k in range(1, n):
            c = remote(tx_ref.at[h, k], rx_ref.at[h, k], tab_s.at[h * n + k], tab_r.at[h * n + k], here.dev(**{AXES[h][0]: k}))
            c.start()
            tabs.append(c)
    moved = here.moved()
    middle = here.middle()
    hot_tab = remote(ht_ref, htr_ref, tab_s.at[0], tab_r.at[0], here.dev(ey=n // 2, ex=n // 2))

    @pl.when(moved)
    def _():
        hot_tab.start()

    @pl.when(jnp.logical_not(moved))
    def _():
        htr_ref[...] = ht_ref[...]

    first = []
    for h in range(2):
        own[h].wait()
        axis = AXES[h][0]
        for i, (s, part, by) in enumerate(((1, 0, 1), (n - 1, 1, -1), (1, 1, 1), (n - 1, 0, -1))):
            c = remote(g_ref.at[h, slot(0, part)], g_ref.at[h, slot(s, part)], g_s.at[h, i], g_r.at[h, i], here.dev(**{axis: by}))
            c.start()
            first.append(c)
    weights = load_weights(0, wg_ref, wu_ref, wd_ref, w_ref, w_sem)
    for c in tabs:
        c.wait_recv()

    def pick(s, start, stop):
        @pl.loop(start, stop)
        def _(m):
            e, h = m // 2, lax.rem(m, 2)
            mat = pick_matrix(rx_ref[h, s, pl.ds(2 * e, 1)], tok_dev)
            picked = dot(mat, g_ref[h, slot(s)]).astype(BF16)
            for j in range(n_dst):
                m_ref[h, rows_at(e * n_row + j * piece + place(s, n) * base_rows, base_rows)] = picked[j * base_rows:(j + 1) * base_rows]

    sends = [[], []]

    def send_rows(e, first_row, size, i, keep):
        for j in range(n_dst - 1, -1 if keep else 0, -1):
            for h in range(2):
                if j:
                    src = m_ref.at[h, pl.ds(e * n_row + j * piece + first_row, size)]
                    dst = m_ref.at[h, pl.ds(recv0 + j * piece + first_row, size)] if e == 0 else re_ref.at[h, pl.ds(j * piece + first_row, size)]
                    c = remote(src, dst, d_s.at[h, e, j, i], d_r.at[h, e, j, i], here.dev(**{AXES[h][1]: j // n_core, 'core': j % n_core}))
                else:
                    dst = m_ref.at[h, pl.ds(recv0, piece)] if e == 0 else re_ref.at[h, pl.ds(0, piece)]
                    c = pltpu.make_async_copy(m_ref.at[h, pl.ds(e * n_row, piece)], dst, d_s.at[h, e, j, i])
                c.start()
                sends[e].append(c)

    pick(0, 0, 2 * exp_dev)
    far = []
    for i, (s, part, by) in enumerate(((1, 0, 1), (n - 1, 1, -1))):
        for h in range(2):
            first[h * 4 + i].wait_recv()
            c = remote(g_ref.at[h, slot(s, part)], g_ref.at[h, slot(far_slot, part)], g_s.at[h, 4 + i], g_r.at[h, 4 + i], here.dev(**{AXES[h][0]: by}))
            c.start()
            far.append(c)
    for i, s in enumerate((1, n - 1)):
        for h in range(2):
            first[h * 4 + 2 + i].wait_recv()
        pick(s, 0, 2 * exp_dev)
    send_rows(0, 0, piece - base_rows, 0, False)
    for c in far:
        c.wait_recv()
    pick(far_slot, 0, 2)
    send_rows(0, piece - base_rows, base_rows, 1, True)

    pick(far_slot, 2, 2 * exp_dev)
    send_rows(1, 0, piece, 0, True)

    hot = [remote(g_ref.at[h, slot(far_slot)], hb_ref.at[h], hot_s.at[h], hot_r.at[h], here.dev(**{AXES[h][1]: n // 2})) for h in range(2)]

    @pl.when(middle)
    def _():
        for c in hot:
            c.start()

    def done_send(c):
        if c.is_remote:
            c.wait_send()

    def done_recv(c):
        if c.is_remote:
            c.wait_recv()
        else:
            c.wait()

    for c in weights:
        c.wait()
    for c in sends[0]:
        done_recv(c)
    base_ffn(here, m_ref, recv0, q_ref.at[0], w_ref, d_model, d_ff, base_rows, ret_s.at[0], ret_r.at[0])

    weights = load_weights(exp_dev - 1, wg_ref, wu_ref, wd_ref, w_ref, w_sem)
    for c in sends[1]:
        done_recv(c)
        done_send(c)
    x_in = pltpu.make_async_copy(re_ref, m_ref.at[:, pl.ds(n_row, n_row)], x_sem)
    x_in.start()
    x_in.wait()
    for c in weights:
        c.wait()
    base_ffn(here, m_ref, n_row, q_ref.at[1], w_ref, d_model, d_ff, base_rows, ret_s.at[1], ret_r.at[1])

    @pl.when(jnp.logical_not(moved))
    def _():
        for h in range(2):
            hb_ref[h] = g_ref[h, slot(0)]

    @pl.when(moved)
    def _():
        hot_tab.wait_recv()
        for c in hot:
            c.wait_recv()

    for c in sends[0]:
        done_send(c)

    def hot_pick(rel):
        @pl.loop(0, exp_dev)
        def _(e):
            mat = pick_matrix(htr_ref[pl.ds(rel * exp_dev + e, 1)], tok_dev)
            for h in range(2):
                m_ref[h, rows_at(rel * hot_dev + e * hot_rows, hot_rows)] = dot(mat, hb_ref[h]).astype(BF16)

    away, here_rows = pl.ds(hot_dev, hot_dev), pl.ds(land, hot_dev)
    hot_pick(1)
    swap = [remote(m_ref.at[h, away], m_ref.at[h, here_rows], swap_s.at[h], swap_r.at[h], here.dev(core=1)) for h in range(2)]
    back = [remote(m_ref.at[h, here_rows], hy_ref.at[h], swap_s.at[2 + h], swap_r.at[2 + h], here.dev(core=1)) for h in range(2)]
    for c in swap:
        c.start()
    hot_pick(0)
    for c in swap:
        c.wait_recv()
    tiles = hot_rows // piece

    @pl.loop(0, exp_dev)
    def _(i):
        e = exp_dev - 1 - i

        @pl.when(i > 0)
        def _():
            for c in load_weights(e, wg_ref, wu_ref, wd_ref, w_ref, w_sem):
                c.wait()

        @pl.loop(0, n_core * tiles)
        def _(k):
            @pl.when((i == exp_dev - 1) & (k == tiles))
            def _():
                for c in back:
                    c.start()

            rows = rows_at((1 - k // tiles) * land + e * hot_rows + lax.rem(k, tiles) * piece, piece)
            y1, y2 = gated_mlp(m_ref[0, rows], m_ref[1, rows], w_ref, d_model, d_ff)
            m_ref[0, rows] = y1
            m_ref[1, rows] = y2

    for h in range(2):
        return_keep(h, m_ref, recv0, q_ref.at[0], ret_s.at[0], piece).wait()
        for j in range(1, n_dst):
            c = return_copy(here, h, j, m_ref, recv0, q_ref.at[0], ret_s.at[0], ret_r.at[0], piece)
            c.wait_send()
            c.wait_recv()
    q_in = pltpu.make_async_copy(q_ref.at[0], m_ref.at[:, pl.ds(recv0, n_row)], x_sem)
    q_in.start()

    for c in swap:
        c.wait_send()
    hy_in = [pltpu.make_async_copy(hy_ref.at[h], m_ref.at[h, away], own_sem.at[h]) for h in range(2)]
    for h in range(2):
        back[h].wait_recv()
        hy_in[h].start()
    for c in hy_in:
        c.wait()
    kinds = n_core * exp_dev

    @pl.loop(0, 2)
    def _(h):
        acc = None
        for k in range(kinds):
            rows = scaled_rows(m_ref[h, pl.ds(k * hot_rows, hot_rows)], htr_ref[kinds + k:kinds + k + 1])
            term = dot(spread_matrix(htr_ref[k:k + 1], tok_dev), rows)
            acc = term if acc is None else acc + term
        hb_ref[h] = acc.astype(BF16)

    sums = [remote(hb_ref.at[h], hs_ref.at[h], sum_s.at[h], sum_r.at[h], here.dev(**{AXES[h][1]: n // 2})) for h in range(2)]

    @pl.when(moved)
    def _():
        for c in sums:
            c.start()

    for h in range(2):
        for i, by in enumerate((-1, 1)):
            pl.semaphore_signal(free_sem.at[h, i], inc=1, device_id=here.dev(**{AXES[h][0]: by}), device_id_type=MESH)

    for c in first + far:
        c.wait_send()

    @pl.when(middle)
    def _():
        for c in hot:
            c.wait_send()

    def load_piece(h, j):
        rows = pl.ds(j * piece, piece)
        return pltpu.make_async_copy(q_ref.at[1, h, rows], g_ref.at[h, rows], load_sem.at[h, j])

    for h in range(2):
        return_keep(h, m_ref, n_row, q_ref.at[1], ret_s.at[1], piece).wait()
        load_piece(h, 0).start()
    for j in range(n_dst - 1, 0, -1):
        for h in range(2):
            return_copy(here, h, j, m_ref, n_row, q_ref.at[1], ret_s.at[1], ret_r.at[1], piece).wait_recv()
            load_piece(h, j).start()
    q_in.wait()
    for h in range(2):
        for j in range(n_dst):
            load_piece(h, j).wait()

    def p_rows(h, s):
        return rows_at((h * n + s) * tok_dev, tok_dev)

    quarter = half // 2

    def quarters(part):
        return [pl.ds((2 * part + q) * quarter, quarter) for q in range(2)]

    def p_part(h, s, part):
        return pl.ds((h * n + s) * tok_dev + part.start, part.size)

    def spread(h, s):
        acc = None
        for e, (ref, start) in enumerate(((m_ref, recv0), (g_ref, 0))):
            rows = jnp.concatenate([ref[h, pl.ds(start + j * piece + place(s, n) * base_rows, base_rows)] for j in range(n_dst)], axis=0)
            term = dot(spread_matrix(rx_ref[h, s, pl.ds(2 * e, 1)], tok_dev), scaled_rows(rows, rx_ref[h, s, pl.ds(2 * e + 1, 1)]))
            acc = term if acc is None else acc + term
        return acc

    ring = []

    def send(h, i, s, part, dst, by, start=True):
        c = remote(w_ref.at[p_part(h, s, part)], dst, ring_s.at[h, i], ring_r.at[h, i], here.dev(**{AXES[h][0]: by}))
        if start:
            c.start()
        ring.append(c)
        return c

    tops = [[], []]
    for h in range(2):
        w_ref[p_rows(h, far_slot)] = spread(h, far_slot).astype(BF16)
        for q in range(2):
            tops[h].append(send(h, q, far_slot, quarters(0)[q], m_ref.at[h, quarters(0)[q]], 1, False))
            tops[h].append(send(h, 2 + q, far_slot, quarters(1)[q], m_ref.at[h, quarters(1)[q]], -1, False))

        for i in range(2):
            pl.semaphore_wait(free_sem.at[h, i], 1)

        @pl.when(jnp.logical_not(middle))
        def _():
            for c in tops[h]:
                c.start()

    last = []
    for s, part, by in ((n - 1, 1, 1), (1, 0, -1)):
        @pl.loop(0, 2)
        def _(h):
            w_ref[p_rows(h, s)] = spread(h, s).astype(BF16)

        for h in range(2):
            last.append(send(h, 4 + part, s, (lo, hi)[part], v_ref.at[h, 1 - part, (lo, hi)[part]], by))

    def add_to(h, s, part, start=0):
        rows = p_part(h, s, part)
        more = m_ref[h, pl.ds(start + part.start, part.size)]
        w_ref[rows] = (w_ref[rows].astype(F32) + more.astype(F32)).astype(BF16)

    @pl.when(middle)
    def _():
        loads = [pltpu.make_async_copy(hs_ref.at[h], m_ref.at[h, pl.ds(hot_dev, tok_dev)], own_sem.at[h]) for h in range(2)]
        for h in range(2):
            sums[h].wait_recv()
            loads[h].start()
        for h in range(2):
            loads[h].wait()
            for q in range(2):
                add_to(h, far_slot, quarters(0)[q], hot_dev)
                tops[h][2 * q].start()
                add_to(h, far_slot, quarters(1)[q], hot_dev)
                tops[h][2 * q + 1].start()

    own_hot = jnp.where(moved, 0.0, 1.0).astype(F32)

    @pl.loop(0, 2)
    def _(h):
        w_ref[p_rows(h, 0)] = (spread(h, 0) + own_hot * hb_ref[h].astype(F32)).astype(BF16)

    out = [pltpu.make_async_copy(w_ref.at[p_rows(h, 0)], p0_ref.at[h], own_sem.at[h]) for h in range(2)]
    for c in out:
        c.start()
    for q in range(2):
        for h in range(2):
            tops[h][2 * q].wait_recv()
            add_to(h, n - 1, quarters(0)[q])
            last.append(send(h, 6 + q, n - 1, quarters(0)[q], v_ref.at[h, 0, quarters(0)[q]], 1))
            tops[h][2 * q + 1].wait_recv()
            add_to(h, 1, quarters(1)[q])
            last.append(send(h, 8 + q, 1, quarters(1)[q], v_ref.at[h, 1, quarters(1)[q]], -1))

    for c in out:
        c.wait()
    for c in tabs + back:
        c.wait_send()
    for h in range(2):
        for j in range(1, n_dst):
            return_copy(here, h, j, m_ref, n_row, q_ref.at[1], ret_s.at[1], ret_r.at[1], piece).wait_send()

    @pl.when(moved)
    def _():
        hot_tab.wait_send()
        for c in sums:
            c.wait_send()

    for c in ring:
        c.wait_send()
    for c in last:
        c.wait_recv()


def layer(n, n_core, base_rows, hot_rows, tokens, tx, ht, w_gate, w_up, w_down):
    tok_dev, d_model = tokens.shape
    exp_dev, _, d_ff = w_gate.shape
    dh = d_model // 2
    n_dst = n * n_core
    n_row = n_dst * n * base_rows
    any_ = pl.BlockSpec(memory_space=pl.ANY)
    vm = pl.BlockSpec(memory_space=pltpu.VMEM)
    dma = pltpu.SemaphoreType.DMA
    hbm = lambda *shape: jax.ShapeDtypeStruct(shape, BF16)
    return pl.pallas_call(
        functools.partial(layer_kernel, n, n_core, exp_dev, base_rows, hot_rows),
        out_shape=(hbm(2, tok_dev, dh), hbm(2, 2, tok_dev, dh), hbm(2, n_row, dh), hbm(exp_dev, 2, n_row, dh), hbm(2, tok_dev, dh), hbm(2, exp_dev * hot_rows, dh)),
        in_specs=[any_, vm, vm, any_, any_, any_],
        out_specs=(any_,) * 6,
        scratch_shapes=[
            pltpu.VMEM(tx.shape, F32),
            pltpu.VMEM(ht.shape, F32),
            pltpu.VMEM((2, n * tok_dev, dh), BF16),
            pltpu.VMEM((2, tok_dev, dh), BF16),
            pltpu.VMEM((2, (exp_dev + 1) * n_row + exp_dev * hot_rows, dh), BF16),
            pltpu.VMEM((max(2 * d_model + 2 * d_ff, 2 * n * tok_dev), dh), BF16),
            dma((2,)), dma((4,)), dma((2 * n,)), dma((2 * n,)), dma((2, 6)), dma((2, 6)),
            dma((2, exp_dev, n_dst, 2)), dma((2, exp_dev, n_dst, 2)), dma((2,)), dma((2,)), dma((4,)), dma((4,)), dma,
            dma((exp_dev, 2, n_dst)), dma((exp_dev, 2, n_dst)), dma((2,)), dma((2,)), dma((2, 10)), dma((2, 10)), dma((2, n_dst)), pltpu.SemaphoreType.REGULAR((2, 2)),
        ],
        compiler_params=pltpu.CompilerParams(vmem_limit_bytes=VMEM_LIMIT, collective_id=0, has_side_effects=True),
        name='layer',
    )(tokens, tx, ht, w_gate, w_up, w_down)[:2]


def last_sum_kernel(p_ref, v_ref, out_ref):
    dh = p_ref.shape[-1]
    for h in range(2):
        out_ref[:, h * dh:(h + 1) * dh] = (p_ref[h].astype(F32) + v_ref[h, 0].astype(F32) + v_ref[h, 1].astype(F32)).astype(BF16)


def last_sum(p0, v):
    _, tok_dev, dh = p0.shape
    steps = 6
    rows = tok_dev // steps
    return pl.pallas_call(
        last_sum_kernel,
        grid=(steps,),
        out_shape=jax.ShapeDtypeStruct((tok_dev, 2 * dh), BF16),
        in_specs=[pl.BlockSpec((2, rows, dh), lambda i: (0, i, 0)), pl.BlockSpec((2, 2, rows, dh), lambda i: (0, 0, i, 0))],
        out_specs=pl.BlockSpec((rows, 2 * dh), lambda i: (i, 0)),
        name='last_sum',
    )(p0, v)


def solution(mesh):
    grid_y = mesh.shape['ey']
    grid_x = mesh.shape['ex']
    n_core = mesh.shape['core']
    n = grid_x
    n_dev = grid_y * grid_x * n_core
    chip_list = target_chips(grid_y, grid_x)

    def device_body(tokens, expert_ids, gate_prob, w_gate, w_up, w_down):
        tok_dev, top_k = expert_ids.shape
        exp_dev = w_gate.shape[0]
        exp_chip = exp_dev * n_core
        n_exp = exp_dev * n_dev
        n_copy = tok_dev * top_k
        base_rows = 2 * n_copy // (3 * n_exp)
        hot_rows = grid_y * grid_x * base_rows // 2
        core = lax.axis_index('core')
        iy = lax.axis_index('ey')
        ix = lax.axis_index('ex')
        dst_chip = jnp.where(is_moved(iy, ix, n), lax.rem(iy + n // 2, n) * n + lax.rem(ix + n // 2, n), iy * n + ix)

        key = expert_ids.reshape(n_copy) * n_copy + jnp.arange(n_copy, dtype=jnp.int32)
        skey, sgate = lax.sort((key, gate_prob.reshape(n_copy)), num_keys=1, is_stable=False)
        stok = (lax.rem(skey, n_copy) // top_k).astype(F32)
        tab = jnp.stack([stok, sgate])
        lo = dst_chip * exp_chip
        hot_shift = hot_rows * exp_chip // base_rows
        by_block = tab.reshape(2, n_copy // base_rows, base_rows)
        e_id = jnp.arange(n_exp)[None, :, None]
        base = jnp.where(e_id < lo, by_block[:, :n_exp], by_block[:, hot_shift:hot_shift + n_exp])
        hot = lax.dynamic_slice(tab, (0, lo * base_rows), (2, exp_chip * (base_rows + hot_rows)))
        hot = hot.reshape(2, exp_chip, base_rows + hot_rows)
        base = lax.dynamic_update_slice(base, hot[:, :, :base_rows], (0, lo, 0))
        base = base.reshape(2, n, n, n_core, exp_dev, base_rows)
        base = lax.dynamic_slice_in_dim(jnp.concatenate([base, base], axis=1), iy, n, axis=1)
        base = lax.dynamic_slice_in_dim(jnp.concatenate([base, base], axis=2), ix, n, axis=2)
        base = jnp.where(core == 0, base, base[:, :, :, ::-1])
        hot = hot[:, :, base_rows:].reshape(2, n_core, exp_dev, hot_rows)
        hot = jnp.where(core == 0, hot, hot[:, ::-1])
        n_row = n * n_core * base_rows
        tx = jnp.stack([base.transpose(2, 4, 0, 1, 3, 5).reshape(n, exp_dev * 2, n_row), base.transpose(1, 4, 0, 2, 3, 5).reshape(n, exp_dev * 2, n_row)])
        tx = jnp.pad(tx, ((0, 0), (0, 0), (0, 8 - exp_dev * 2), (0, 0)))
        ht = hot.reshape(2 * exp_chip, hot_rows)

        p0, v = layer(n, n_core, base_rows, hot_rows, tokens, tx, ht, w_gate, w_up, w_down)
        return last_sum(p0, v)

    return jax.shard_map(device_body, mesh=mesh, in_specs=(TOKEN_SPEC, TOKEN_SPEC, TOKEN_SPEC, EXPERT_SPEC, EXPERT_SPEC, EXPERT_SPEC), out_specs=TOKEN_SPEC, check_vma=False)
```
